32 devices in a mesh: dp: 2 (over x), section: 4 (over y, core), tensor: 4 (over z).
Axes of the slice: x: 2, y: 2, z: 4, core: 2. Of those that a mesh axis runs over, the one named last changes fastest.
Arguments:
- failed_section: int32 [2], P('dp'), may hold values from 0 to 999
- token_ids: int32 [2, 2048], P('dp'), may hold values from 0 to 100001, as said below
- section_outputs: bfloat16 [2, 4, 2048, 2048], P('dp', 'section', None, 'tensor'), may hold values from -11 to 11
- w_query: float32 [4, 2048, 1024], P('section', 'dp', 'tensor'), may hold values from -1 to 1
- w_key: float32 [4, 2048, 1024], P('section', 'dp', 'tensor'), may hold values from -2 to 2
- w_value: float32 [4, 2048, 1024], P('section', 'dp', 'tensor'), may hold values from -0.125 to 0.125
- w_out: float32 [4, 2048, 1024], P('section', 'dp', 'tensor'), may hold values from -0.75 to 0.75
- m_value: float32 [4, 2048, 1024], P('section', 'dp', 'tensor'), may hold values from -3 to 3
- v_value: float32 [4, 2048, 1024], P('section', 'dp', 'tensor'), may hold values from 0.001 to 1
- m_out: float32 [4, 2048, 1024], P('section', 'dp', 'tensor'), may hold values from -3 to 3
- v_out: float32 [4, 2048, 1024], P('section', 'dp', 'tensor'), may hold values from 0.001 to 1
Outputs:
- restored_query: float32 [2, 4, 2048, 1024], P('dp', 'section', None, 'tensor')
- restored_key: float32 [2, 4, 2048, 1024], P('dp', 'section', None, 'tensor')
- restored_value: float32 [2, 4, 2048, 1024], P('dp', 'section', None, 'tensor')
- restored_out: float32 [2, 4, 2048, 1024], P('dp', 'section', None, 'tensor')
- restored_m_value: float32 [2, 4, 2048, 1024], P('dp', 'section', None, 'tensor')
- restored_v_value: float32 [2, 4, 2048, 1024], P('dp', 'section', None, 'tensor')
- restored_m_out: float32 [2, 4, 2048, 1024], P('dp', 'section', None, 'tensor')
- restored_v_out: float32 [2, 4, 2048, 1024], P('dp', 'section', None, 'tensor')
- attn_update: bfloat16 [2, 4, 2048, 2048], P('dp', 'section', None, 'tensor')
The draws below stay inside these ranges and needn't reach their ends.
Inputs may be any that keep to these rules, and one draw needn't show every extreme that they name: `token_ids`: token ids of each replica's micro-batch; the id 100001 ends a document, the others are ordinary tokens below 100000.
All inputs are finite; a program needn't handle non-finite values.
Results may differ from the reference program's by a relative error of at most 0.0087.
Values may be sent and summed in bfloat16 or wider, within the bound.
A program may use at most 128 MiB of HBM per device.

```python
import math
import jax
import jax.numpy as jnp
from jax import lax

D = 2048
HD = 128
HEADS = 8
TOKENS = 2048
INNER = 1024
REPLICAS = 2
SECTIONS = 4


def draw_token_ids(key, part):
    word_ids = jax.random.randint(jax.random.fold_in(key, 11), (REPLICAS, TOKENS), 0, 100000)
    doc_marks = jax.random.randint(jax.random.fold_in(key, 12), (REPLICAS, TOKENS), 0, max(2, TOKENS // 8))
    return jnp.where(doc_marks == 0, 100001, word_ids).astype(jnp.int32)


def draw_section_outputs(key, part):
    full_shape = (REPLICAS, SECTIONS, TOKENS, D)
    entries = jnp.clip(jax.random.normal(jax.random.fold_in(key, 23), full_shape, jnp.float32), -6.0, 6.0)
    return entries.astype(jnp.bfloat16)


def projection_pair(key):
    full_shape = (SECTIONS, D, INNER)
    leading = jnp.clip(jax.random.normal(jax.random.fold_in(key, 31), full_shape, jnp.float32), -6.0, 6.0) / math.sqrt(D)
    other = jnp.clip(jax.random.normal(jax.random.fold_in(key, 32), full_shape, jnp.float32), -6.0, 6.0) / math.sqrt(D)
    second = other
    return (leading, second)


def draw_w_query(key, part):
    return projection_pair(key)[0].astype(jnp.float32)


def draw_w_key(key, part):
    return projection_pair(key)[1].astype(jnp.float32)


def block_levels(rng, dims, pieces, least, top_value):
    level, own = 1.0, jax.random.fold_in(rng, 6)
    for dim, parts in pieces:
        draws = jnp.exp(jax.random.uniform(jax.random.fold_in(own, dim), (parts,), jnp.float32, least / len(pieces), top_value / len(pieces)))
        level = level * jnp.repeat(draws, dims[dim] // parts).reshape([-1 if axis == dim else 1 for axis in range(len(dims))])
    return level


def bell_draw(rng, shape, deviation, limit, cuts=(), held_as=jnp.bfloat16):
    drawn = jax.random.normal(rng, shape, jnp.float32) * deviation
    if len(cuts) > 0:
        drawn = block_levels(rng, shape, cuts, -0.22, 0.18) * drawn
    return jnp.clip(drawn, min=-limit, max=limit).astype(held_as)


def setup_inputs(seed: int = 0) -> dict:
    arg_keys = jax.random.split(jax.random.key(seed), 12)
    return {
        "failed_section": jax.random.randint(arg_keys[0], (REPLICAS,), 0, 1000).astype(jnp.int32),
        "token_ids": draw_token_ids(jax.random.fold_in(arg_keys[11], 71), 0),
        "section_outputs": draw_section_outputs(jax.random.fold_in(arg_keys[11], 71), 0),
        "w_query": draw_w_query(jax.random.fold_in(arg_keys[11], 71), 0),
        "w_key": draw_w_key(jax.random.fold_in(arg_keys[11], 71), 0),
        "w_value": bell_draw(arg_keys[5], (SECTIONS, D, INNER), D ** -0.5, 0.125, ((0, 4), (1, 2), (2, 4)), jnp.float32),
        "w_out": bell_draw(arg_keys[6], (SECTIONS, D, INNER), (INNER // 16) ** -0.5, 0.75, ((0, 4), (1, 2), (2, 4)), jnp.float32),
        "m_value": bell_draw(arg_keys[7], (SECTIONS, D, INNER), 0.5, 3.0, ((0, 4), (1, 2), (2, 4)), jnp.float32),
        "v_value": jnp.clip(jnp.exp(math.log(1.0) - 6.9077552 * jax.random.uniform(arg_keys[8], (SECTIONS, D, INNER), jnp.float32) ** block_levels(arg_keys[8], (SECTIONS, D, INNER), ((0, 4), (1, 2), (2, 4)), -0.2, 0.2)), 0.001, 1.0),
        "m_out": bell_draw(arg_keys[9], (SECTIONS, D, INNER), 0.5, 3.0, ((0, 4), (1, 2), (2, 4)), jnp.float32),
        "v_out": jnp.clip(jnp.exp(math.log(1.0) - 6.9077552 * jax.random.uniform(arg_keys[10], (SECTIONS, D, INNER), jnp.float32) ** block_levels(arg_keys[10], (SECTIONS, D, INNER), ((0, 4), (1, 2), (2, 4)), -0.2, 0.2)), 0.001, 1.0),
    }


end_token = 100001
mask_fill = -1e+30

def document_ids(token_row):
    doc_ends = (token_row == end_token).astype(jnp.int32)
    return jnp.cumsum(doc_ends) - doc_ends

def attend_head(query_head, key_head, value_head, allowed):
    scores = jnp.dot(query_head, key_head.T, preferred_element_type=jnp.float32) * (1.0 / math.sqrt(HD))
    scores = jnp.where(allowed, scores, mask_fill)
    highest = lax.optimization_barrier(jnp.max(scores, axis=1, keepdims=True))
    weights = jnp.exp(scores - highest)
    probs = (weights / lax.optimization_barrier(jnp.sum(weights, axis=1, keepdims=True))).astype(jnp.bfloat16)
    return jnp.dot(probs, value_head, preferred_element_type=jnp.float32).astype(jnp.bfloat16)

def recompute(incoming, token_row, query_master, key_master, value_master, out_master):
    queries = jnp.dot(incoming, query_master.astype(jnp.bfloat16), preferred_element_type=jnp.float32).astype(jnp.bfloat16)
    key_vals = jnp.dot(incoming, key_master.astype(jnp.bfloat16), preferred_element_type=jnp.float32).astype(jnp.bfloat16)
    value_vals = jnp.dot(incoming, value_master.astype(jnp.bfloat16), preferred_element_type=jnp.float32).astype(jnp.bfloat16)
    query_heads = queries.reshape(TOKENS, HEADS, HD).transpose(1, 0, 2)
    key_heads = key_vals.reshape(TOKENS, HEADS, HD).transpose(1, 0, 2)
    value_heads = value_vals.reshape(TOKENS, HEADS, HD).transpose(1, 0, 2)
    document = document_ids(token_row)
    positions = jnp.arange(TOKENS)
    allowed = (positions[None, :] <= positions[:, None]) & (document[None, :] == document[:, None])
    context = lax.map(lambda trio: attend_head(trio[0], trio[1], trio[2], allowed), (query_heads, key_heads, value_heads))
    context = context.transpose(1, 0, 2).reshape(TOKENS, INNER)
    return jnp.dot(context, out_master.astype(jnp.bfloat16).T, preferred_element_type=jnp.float32).astype(jnp.bfloat16)

def reference(failed_section, token_ids, section_outputs, w_query, w_key, w_value, w_out, m_value, v_value, m_out, v_out):
    sources = (w_query, w_key, w_value, w_out, m_value, v_value, m_out, v_out)
    results = [jnp.zeros((REPLICAS, SECTIONS, D, INNER), jnp.float32) for item in sources]
    update_all = jnp.zeros((REPLICAS, SECTIONS, TOKENS, D), jnp.bfloat16)
    for replica in range(REPLICAS):
        section_failed = jnp.remainder(failed_section[replica], SECTIONS).astype(jnp.int32)
        before = jnp.remainder(section_failed + SECTIONS - 1, SECTIONS).astype(jnp.int32)
        incoming = section_outputs[replica, before]
        blocks = [source[section_failed] for source in sources]
        update = recompute(incoming, token_ids[replica], blocks[0], blocks[1], blocks[2], blocks[3])
        results = [result.at[replica, section_failed].set(block) for result, block in zip(results, blocks)]
        update_all = update_all.at[replica, section_failed].set(update)
    return (results[0], results[1], results[2], results[3], results[4], results[5], results[6], results[7], update_all)
```

```python
import math

import jax
import jax.numpy as jnp
from jax import lax
from jax.experimental import pallas as pl
from jax.experimental.pallas import tpu as pltpu
from jax.sharding import PartitionSpec as P

HD = 128


end_token = 100001
mask_fill = -1e30


def passed_along(array, axis, by):
    count = lax.axis_size(axis)
    return lax.ppermute(array, axis, [(i, (i + by) % count) for i in range(count)])


def document_ids(token_row):
    doc_ends = (token_row == end_token).astype(jnp.int32)
    return jnp.cumsum(doc_ends) - doc_ends


def attend(queries, key_vals, value_vals, token_row):
    token_count = queries.shape[0]
    heads_local = queries.shape[1] // HD
    block_rows = min(512, token_count)
    document = document_ids(token_row)
    positions = jnp.arange(token_count, dtype=jnp.int32)
    key_heads = key_vals.reshape(token_count, heads_local, HD)
    value_heads = value_vals.reshape(token_count, heads_local, HD)

    def one_block(block_index):
        first_row = block_index * block_rows
        query_block = lax.dynamic_slice_in_dim(queries, first_row, block_rows, 0).reshape(
            block_rows, heads_local, HD
        )
        scores = jnp.einsum(
            "qhd,khd->hqk", query_block, key_heads, preferred_element_type=jnp.float32
        ) * (1.0 / math.sqrt(HD))
        query_pos = lax.dynamic_slice_in_dim(positions, first_row, block_rows, 0)
        query_doc = lax.dynamic_slice_in_dim(document, first_row, block_rows, 0)
        allowed = (positions[None, :] <= query_pos[:, None]) & (
            document[None, :] == query_doc[:, None]
        )
        scores = jnp.where(allowed[None], scores, mask_fill)
        highest = jnp.max(scores, axis=2, keepdims=True)
        weights = jnp.exp(scores - highest)
        probs = (weights / jnp.sum(weights, axis=2, keepdims=True)).astype(jnp.bfloat16)
        context = jnp.einsum(
            "hqk,khd->qhd", probs, value_heads, preferred_element_type=jnp.float32
        ).astype(jnp.bfloat16)
        return context.reshape(block_rows, heads_local * HD)

    blocks = lax.map(one_block, jnp.arange(token_count // block_rows, dtype=jnp.int32))
    return blocks.reshape(token_count, heads_local * HD)


def shards(
    failed_section,
    token_ids,
    section_outputs,
    w_query,
    w_key,
    w_value,
    w_out,
    m_value,
    v_value,
    m_out,
    v_out,
):
    section_failed = jnp.remainder(failed_section[0], lax.axis_size("section"))
    replacing = lax.axis_index("section") == section_failed
    states = (
        lax.all_gather(w_query, "dp", axis=1, tiled=True),
        lax.all_gather(w_key, "dp", axis=1, tiled=True),
        lax.all_gather(w_value, "dp", axis=1, tiled=True),
        lax.all_gather(w_out, "dp", axis=1, tiled=True),
        lax.all_gather(m_value, "dp", axis=1, tiled=True),
        lax.all_gather(v_value, "dp", axis=1, tiled=True),
        lax.all_gather(m_out, "dp", axis=1, tiled=True),
        lax.all_gather(v_out, "dp", axis=1, tiled=True),
    )
    masters = states[:4]
    moments = states[4:]
    query_bf = masters[0][0].astype(jnp.bfloat16)
    key_bf = masters[1][0].astype(jnp.bfloat16)
    value_bf = masters[2][0].astype(jnp.bfloat16)
    out_bf = masters[3][0].astype(jnp.bfloat16)
    inner_local = query_bf.shape[1]
    w_joined = jnp.concatenate([query_bf, key_bf, value_bf], axis=1)
    incoming = passed_along(section_outputs, "section", 1)
    projected = jnp.dot(
        lax.all_gather(incoming, "tensor", axis=3, tiled=True)[0, 0],
        w_joined,
        preferred_element_type=jnp.float32,
    )
    queries = projected[:, :inner_local].astype(jnp.bfloat16)
    key_vals = projected[:, inner_local : 2 * inner_local].astype(jnp.bfloat16)
    value_vals = projected[:, 2 * inner_local :].astype(jnp.bfloat16)
    context = attend(queries, key_vals, value_vals, token_ids[0])
    context_whole = lax.all_gather(context, "tensor", axis=1, tiled=True)
    out_slice = lax.all_to_all(out_bf, "tensor", split_axis=0, concat_axis=1, tiled=True)
    update = lax.dot_general(
        context_whole, out_slice, (((1,), (1,)), ((), ())), preferred_element_type=jnp.float32
    ).astype(jnp.bfloat16)

    def placed(gathered):
        return jnp.where(replacing, gathered[None], jnp.zeros_like(gathered[None]))

    update_block = jnp.where(
        replacing, update[None, None], jnp.zeros((1, 1) + update.shape, jnp.bfloat16)
    )
    return (
        placed(masters[0]),
        placed(masters[1]),
        placed(masters[2]),
        placed(masters[3]),
        placed(moments[0]),
        placed(moments[1]),
        placed(moments[2]),
        placed(moments[3]),
        update_block,
    )


MESH = pl.DeviceIdType.MESH
CHUNKS = 4
STATES = 8


def relay_kernel(
    f_ref,
    f_vec,
    doc_row,
    doc_col,
    acts,
    s0,
    s1,
    s2,
    s3,
    s4,
    s5,
    s6,
    s7,
    state_out,
    context_out,
    out_rows_out,
    f_peer,
    own_f32,
    own_bf,
    pair_bf,
    to_peer,
    held,
    x_own,
    x_pair,
    x_mine,
    x_flip,
    x_all,
    qkv,
    qkv_pair,
    scores,
    ctx,
    ctx_pair,
    rows_mine,
    rows_pair,
    load_x_sem,
    load_s_sem,
    f_sems,
    pair_x_send,
    pair_x_recv,
    flip_send,
    flip_recv,
    pair_s_send,
    pair_s_recv,
    cross_send,
    cross_recv,
    got_send,
    got_recv,
    line_send,
    line_recv,
    over_send,
    over_recv,
    qkv_send,
    qkv_recv,
    ctx_send,
    ctx_recv,
    ctxp_send,
    ctxp_recv,
    rows_send,
    rows_recv,
    rowsp_sems,
    out_sems,
):
    states = (s0, s1, s2, s3, s4, s5, s6, s7)
    replica = lax.axis_index("dp")
    section = lax.axis_index("section")
    rank = lax.axis_index("tensor")
    side = section // 2
    core = section % 2
    other_core = 1 - core
    peer = 1 - replica
    pair_id = {"section": side * 2 + other_core}
    flip_id = {"section": (1 - side) * 2 + core}
    peer_id = {"dp": peer}
    sections = 4
    ranks = ctx.shape[1]
    chunks = x_own.shape[0]
    lane_rows = x_own.shape[1]
    chunk_rows = 2 * lane_rows
    piece = lane_rows // 2
    width = x_own.shape[2]
    half_rows = held.shape[3]
    scale = math.log2(math.e) / math.sqrt(HD)

    def remote(src, dst, send, recv, where_to):
        return pltpu.make_async_remote_copy(
            src_ref=src,
            dst_ref=dst,
            send_sem=send,
            recv_sem=recv,
            device_id=where_to,
            device_id_type=MESH,
        )

    def load_x(k):
        first = pl.multiple_of(k * chunk_rows + core * lane_rows, lane_rows)
        return pltpu.make_async_copy(
            acts.at[pl.ds(first, lane_rows)], x_own.at[k], load_x_sem.at[k]
        )

    def load_s(j):
        return pltpu.make_async_copy(states[j], own_f32.at[j], load_s_sem.at[j])

    def pair_x(k):
        first = pl.multiple_of(k * chunk_rows + other_core * lane_rows, lane_rows)
        return remote(
            acts.at[pl.ds(first, lane_rows)],
            x_pair.at[k],
            pair_x_send.at[k],
            pair_x_recv.at[k],
            pair_id,
        )

    def f_copy():
        return remote(f_vec, f_peer, f_sems.at[0], f_sems.at[1], peer_id)

    def flip_x(k):
        return remote(x_mine.at[k], x_flip.at[k], flip_send.at[k], flip_recv.at[k], flip_id)

    def pair_s(j):
        if j < 3:
            return remote(
                own_bf.at[j], pair_bf.at[j], pair_s_send.at[j], pair_s_recv.at[j], pair_id
            )
        return remote(
            own_bf.at[j, other_core],
            pair_bf.at[j, other_core],
            pair_s_send.at[j],
            pair_s_recv.at[j],
            pair_id,
        )

    def pair_s_arrival(j):
        if j < 3:
            return pair_s(j)
        return remote(
            own_bf.at[j, core],
            pair_bf.at[j, core],
            pair_s_send.at[j],
            pair_s_recv.at[j],
            pair_id,
        )

    def cross(j):
        return remote(
            to_peer.at[j], held.at[replica, j, core], cross_send.at[j], cross_recv.at[j], peer_id
        )

    def cross_arrival(j):
        return remote(
            to_peer.at[j], held.at[peer, j, core], cross_send.at[j], cross_recv.at[j], peer_id
        )

    def got(j):
        return remote(
            held.at[peer, j, core],
            held.at[peer, j, core],
            got_send.at[j],
            got_recv.at[j],
            pair_id,
        )

    def got_arrival(j):
        return remote(
            held.at[peer, j, other_core],
            held.at[peer, j, other_core],
            got_send.at[j],
            got_recv.at[j],
            pair_id,
        )

    mine_rows = pl.ds(pl.multiple_of(side * piece, piece), piece)
    flip_rows = pl.ds(pl.multiple_of((1 - side) * piece, piece), piece)

    def line(k, owner, slot, target):
        part = x_all.at[owner, k, mine_rows]
        return remote(
            part, part, line_send.at[k, slot], line_recv.at[k, owner], {"tensor": target}
        )

    def over(k, owner):
        part = x_all.at[owner, k, mine_rows]
        return remote(part, part, over_send.at[k, owner], over_recv.at[k, owner], flip_id)

    def over_arrival(k, owner):
        part = x_all.at[owner, k, flip_rows]
        return remote(part, part, over_send.at[k, owner], over_recv.at[k, owner], flip_id)

    def qkv_copy(k, lane):
        return remote(
            qkv_pair.at[k], qkv.at[2 * k + lane], qkv_send.at[k], qkv_recv.at[k], pair_id
        )

    def ctx_line(k, owner, slot, target):
        part = ctx.at[k, owner]
        return remote(
            part, part, ctx_send.at[k, slot], ctx_recv.at[k, owner], {"tensor": target}
        )

    def ctx_pair_copy(k):
        return remote(
            ctx.at[k], ctx_pair.at[k], ctxp_send.at[k], ctxp_recv.at[k], pair_id
        )

    def rows_copy(target):
        per_half = half_rows // rows_mine.shape[1]
        first = (target % per_half) * rows_mine.shape[1]
        return remote(
            held.at[target // per_half, 3, core, pl.ds(first, rows_mine.shape[1])],
            rows_mine.at[rank],
            rows_send.at[target],
            rows_recv.at[rank],
            {"tensor": target},
        )

    def rows_arrival(owner):
        return remote(
            rows_mine.at[owner],
            rows_mine.at[owner],
            rows_send.at[owner],
            rows_recv.at[owner],
            {"tensor": owner},
        )

    def rows_pair_copy():
        return remote(rows_mine, rows_pair, rowsp_sems.at[0], rowsp_sems.at[1], pair_id)

    def near(body):
        for slot, step in enumerate((1, -1, 2, -2)):
            target = rank + step

            @pl.when((target >= 0) & (target < ranks))
            def _(slot=slot, target=target):
                body(slot, target)

    def arrivals(body):
        for step in (1, 2, 3):
            for sign in (1, -1):
                owner = rank - sign * step

                @pl.when((owner >= 0) & (owner < ranks))
                def _(owner=owner):
                    body(owner)

    def relayed(body):
        @pl.when(rank == 2)
        def _():
            body(0, 4, 3)

        @pl.when(rank == 1)
        def _():
            body(3, 4, 0)

    f_mine = lax.rem(f_ref[0], sections)
    f_from = lax.rem(f_mine + sections - 1, sections)
    from_core = lax.rem(f_from, 2) == core
    from_side = (f_from // 2) == side
    f_core = lax.rem(f_mine, 2) == core

    for k in range(chunks):
        load_x(k).start()
    for j in range(STATES):
        load_s(j).start()

    barrier = pltpu.get_barrier_semaphore()
    for where_to in (pair_id, flip_id, peer_id):
        pl.semaphore_signal(barrier, inc=1, device_id=where_to, device_id_type=MESH)
    for step in range(1, ranks):
        pl.semaphore_signal(
            barrier,
            inc=1,
            device_id={"tensor": lax.rem(rank + step, ranks)},
            device_id_type=MESH,
        )
    pl.semaphore_wait(barrier, 2 + ranks)

    f_copy().start()
    for k in range(chunks):
        pair_x(k).start()

    def spread(k):
        load_x(k).wait()
        pair_x(k).wait_recv()
        x_mine[k] = jnp.where(from_core, x_own[k], x_pair[k])
        flip_x(k).start()

    def settle(k):
        flip_x(k).wait_recv()
        x_all[rank, k] = jnp.where(from_side, x_mine[k], x_flip[k])
        near(lambda slot, target: line(k, rank, slot, target).start())

    def forward(k):
        def one(owner):
            line(k, owner, 0, owner).wait_recv()
            over(k, owner).start()

        arrivals(one)
        relayed(lambda owner, slot, target: line(k, owner, slot, target).start())

    def forward_ranked(k):
        for step in (1, 2):
            for sign in (1, -1):
                owner = rank - sign * step

                @pl.when((owner >= 0) & (owner < ranks))
                def _(owner=owner):
                    line(k, owner, 0, owner).wait_recv()
                    over(k, owner).start()

        relayed(lambda owner, slot, target: line(k, owner, slot, target).start())
        for sign in (1, -1):
            owner = rank - sign * 3

            @pl.when((owner >= 0) & (owner < ranks))
            def _(owner=owner):
                line(k, owner, 0, owner).wait_recv()
                over(k, owner).start()

    def rounded(j):
        load_s(j).wait()

        @pl.loop(0, half_rows // 128)
        def _(i):
            rows = pl.ds(pl.multiple_of(i * 128, 128), 128)
            own_bf[j, 0, rows] = own_f32[j, rows, :HD].astype(jnp.bfloat16)
            own_bf[j, 1, rows] = own_f32[j, rows, HD:].astype(jnp.bfloat16)

        pair_s(j).start()

    def chosen(j, peer_core):
        pair_s_arrival(j).wait_recv()
        to_peer[j] = jnp.where(peer_core, own_bf[j, core], pair_bf[j, core])
        cross(j).start()
        if j < 3:
            held[replica, j] = jnp.where(f_core, own_bf[j], pair_bf[j])
        if j == 3:
            held[replica, j, core] = jnp.where(f_core, own_bf[j, core], pair_bf[j, core])

    def state_out_copy(j, lane, sem):
        return pltpu.make_async_copy(held.at[peer, j, lane], state_out.at[j, lane], sem)

    def arrived(j):
        cross_arrival(j).wait_recv()
        got(j).start()
        state_out_copy(j, core, out_sems.at[j]).start()

    def paired(j):
        got_arrival(j).wait_recv()
        state_out_copy(j, other_core, out_sems.at[STATES + j]).start()

    def project(k):
        arrivals(lambda owner: over_arrival(k, owner).wait_recv())
        total = None
        per_half = half_rows // width
        for b in range(ranks):
            half, rows = b // per_half, pl.ds((b % per_half) * width, width)
            weight = jnp.concatenate(
                [held[half, j, lane, rows] for j in range(3) for lane in range(2)], axis=1
            )
            part = jnp.dot(x_all[b, k], weight, preferred_element_type=jnp.float32)
            total = part if total is None else total + part
        for j in range(3):
            first = total[:, (2 * j) * HD : (2 * j + 1) * HD].astype(jnp.bfloat16)
            second = total[:, (2 * j + 1) * HD : (2 * j + 2) * HD].astype(jnp.bfloat16)
            qkv[2 * k + core, j] = jnp.where(core == 0, first, second)
            qkv_pair[k, j] = jnp.where(core == 0, second, first)
        qkv_copy(k, core).start()

    def attend_rows(k, lane):
        dims = (((1,), (1,)), ((), ()))
        i = 2 * k + lane
        q = qkv[i, 0]
        docs = doc_col[i]

        def score(b, causal):
            s = lax.dot_general(q, qkv[b, 1], dims, preferred_element_type=jnp.float32)
            allowed = doc_row[b] == docs
            if causal:
                shape = (lane_rows, lane_rows)
                allowed = allowed & (
                    lax.broadcasted_iota(jnp.int32, shape, 1)
                    <= lax.broadcasted_iota(jnp.int32, shape, 0)
                )
            s = jnp.where(allowed, s, mask_fill)
            scores[b] = s
            return jnp.max(s, axis=1, keepdims=True)

        high = score(i, True)
        if i > 0:
            high = lax.fori_loop(
                0, i, lambda b, high: jnp.maximum(high, score(b, False)), high
            )

        def weigh(b, carry):
            total, acc = carry
            weights = jnp.exp2((scores[b] - high) * scale)
            total = total + jnp.sum(weights, axis=1, keepdims=True)
            acc = acc + jnp.dot(
                weights.astype(jnp.bfloat16), qkv[b, 2], preferred_element_type=jnp.float32
            )
            return total, acc

        total, acc = lax.fori_loop(
            0,
            i + 1,
            weigh,
            (jnp.zeros((lane_rows, 1), jnp.float32), jnp.zeros((lane_rows, HD), jnp.float32)),
        )
        ctx[k, rank, lane * lane_rows : (lane + 1) * lane_rows] = (acc / total).astype(
            jnp.bfloat16
        )

    def attend(k):
        qkv_copy(k, other_core).wait_recv()
        for lane in range(2):
            attend_rows(k, lane)
        near(lambda slot, target: ctx_line(k, rank, slot, target).start())

    def context_out_copy(k, lane, source, sem):
        return pltpu.make_async_copy(source.at[k], context_out.at[lane, k], sem)

    def collect(k):
        for step in (1, 2):
            for sign in (1, -1):
                owner = rank - sign * step

                @pl.when((owner >= 0) & (owner < ranks))
                def _(owner=owner):
                    ctx_line(k, owner, 0, owner).wait_recv()

        relayed(lambda owner, slot, target: ctx_line(k, owner, slot, target).start())
        for sign in (1, -1):
            owner = rank - sign * 3

            @pl.when((owner >= 0) & (owner < ranks))
            def _(owner=owner):
                ctx_line(k, owner, 0, owner).wait_recv()

        ctx_pair_copy(k).start()
        context_out_copy(k, core, ctx, out_sems.at[2 * STATES + k]).start()

    def collected(k):
        ctx_pair_copy(k).wait_recv()
        context_out_copy(k, other_core, ctx_pair, out_sems.at[2 * STATES + chunks + k]).start()

    def send_rows():
        for target in range(ranks):

            @pl.when(target != rank)
            def _(target=target):
                rows_copy(target).start()

        for target in range(ranks):

            @pl.when(target == rank)
            def _(target=target):
                per_half = half_rows // rows_mine.shape[1]
                first = (target % per_half) * rows_mine.shape[1]
                rows_mine[target] = held[
                    target // per_half, 3, core, pl.ds(first, rows_mine.shape[1])
                ]

    def rows_out_copy(lane, source, sem):
        return pltpu.make_async_copy(source, out_rows_out.at[lane], sem)

    def take_rows():
        for owner in range(ranks):

            @pl.when(owner != rank)
            def _(owner=owner):
                rows_arrival(owner).wait_recv()

        rows_pair_copy().start()
        rows_out_copy(core, rows_mine, out_sems.at[2 * STATES + 2 * chunks]).start()

    spread(0)
    spread(1)
    for j in range(4):
        rounded(j)
    f_copy().wait_recv()
    peer_core = lax.rem(jnp.max(f_peer[...]).astype(jnp.int32), 2) == core
    settle(0)
    for j in range(4):
        chosen(j, peer_core)
    spread(2)
    settle(1)
    for j in range(4, STATES):
        rounded(j)
    forward_ranked(0)
    for j in range(4, STATES):
        chosen(j, peer_core)
    settle(2)
    spread(3)
    forward_ranked(1)
    for j in range(3):
        arrived(j)
    settle(3)
    for j in range(3):
        paired(j)
    project(0)
    forward_ranked(2)
    attend(0)
    arrived(3)
    send_rows()
    project(1)
    forward_ranked(3)
    attend(1)
    collect(0)
    project(2)
    attend(2)
    arrived(4)
    arrived(5)
    collect(1)
    project(3)
    attend(3)
    take_rows()
    arrived(6)
    arrived(7)
    for j in range(3, STATES):
        paired(j)
    for k in range(2, chunks):
        collect(k)
    rows_pair_copy().wait_recv()
    rows_out_copy(other_core, rows_pair, out_sems.at[2 * STATES + 2 * chunks + 1]).start()
    for k in range(chunks):
        collected(k)

    f_copy().wait_send()
    for k in range(chunks):
        pair_x(k).wait_send()
        flip_x(k).wait_send()
        near(lambda slot, target: line(k, rank, slot, target).wait_send())
        relayed(lambda owner, slot, target: line(k, owner, slot, target).wait_send())
        arrivals(lambda owner: over(k, owner).wait_send())
        qkv_copy(k, core).wait_send()
        near(lambda slot, target: ctx_line(k, rank, slot, target).wait_send())
        relayed(lambda owner, slot, target: ctx_line(k, owner, slot, target).wait_send())
        ctx_pair_copy(k).wait_send()
        context_out_copy(k, core, ctx, out_sems.at[2 * STATES + k]).wait()
        context_out_copy(k, other_core, ctx_pair, out_sems.at[2 * STATES + chunks + k]).wait()
    for j in range(STATES):
        pair_s(j).wait_send()
        cross(j).wait_send()
        got(j).wait_send()
        state_out_copy(j, core, out_sems.at[j]).wait()
        state_out_copy(j, other_core, out_sems.at[STATES + j]).wait()
    for target in range(ranks):

        @pl.when(target != rank)
        def _(target=target):
            rows_copy(target).wait_send()

    rows_pair_copy().wait_send()
    rows_out_copy(core, rows_mine, out_sems.at[2 * STATES + 2 * chunks]).wait()
    rows_out_copy(other_core, rows_pair, out_sems.at[2 * STATES + 2 * chunks + 1]).wait()


def relay_call(failed, document, acts, states, ranks):
    tokens, width = acts.shape
    half_rows, inner_local = states[0].shape
    chunks = CHUNKS
    lane_rows = tokens // (2 * chunks)
    blocks = 2 * chunks
    out_width = 2 * half_rows // ranks
    bf, f32 = jnp.bfloat16, jnp.float32
    vmem, dma = pltpu.VMEM, pltpu.SemaphoreType.DMA
    anywhere = pl.BlockSpec(memory_space=pl.ANY)
    in_vmem = pl.BlockSpec(memory_space=pltpu.VMEM)
    return pl.pallas_call(
        relay_kernel,
        out_shape=(
            jax.ShapeDtypeStruct((STATES, 2, half_rows, HD), bf),
            jax.ShapeDtypeStruct((2, chunks, ranks, 2 * lane_rows, HD), bf),
            jax.ShapeDtypeStruct((2, ranks, out_width, HD), bf),
        ),
        in_specs=[pl.BlockSpec(memory_space=pltpu.SMEM), in_vmem, in_vmem, in_vmem]
        + [anywhere] * (1 + STATES),
        out_specs=(anywhere,) * 3,
        scratch_shapes=[
            vmem((8, 128), f32),
            vmem((STATES, half_rows, inner_local), f32),
            vmem((STATES, 2, half_rows, HD), bf),
            vmem((STATES, 2, half_rows, HD), bf),
            vmem((STATES, half_rows, HD), bf),
            vmem((2, STATES, 2, half_rows, HD), bf),
            vmem((chunks, lane_rows, width), bf),
            vmem((chunks, lane_rows, width), bf),
            vmem((chunks, lane_rows, width), bf),
            vmem((chunks, lane_rows, width), bf),
            vmem((ranks, chunks, lane_rows, width), bf),
            vmem((blocks, 3, lane_rows, HD), bf),
            vmem((chunks, 3, lane_rows, HD), bf),
            vmem((blocks, lane_rows, lane_rows), f32),
            vmem((chunks, ranks, 2 * lane_rows, HD), bf),
            vmem((chunks, ranks, 2 * lane_rows, HD), bf),
            vmem((ranks, out_width, HD), bf),
            vmem((ranks, out_width, HD), bf),
            dma((chunks,)),
            dma((STATES,)),
            dma((2,)),
            dma((chunks,)),
            dma((chunks,)),
            dma((chunks,)),
            dma((chunks,)),
            dma((STATES,)),
            dma((STATES,)),
            dma((STATES,)),
            dma((STATES,)),
            dma((STATES,)),
            dma((STATES,)),
            dma((chunks, 5)),
            dma((chunks, ranks)),
            dma((chunks, ranks)),
            dma((chunks, ranks)),
            dma((chunks,)),
            dma((chunks,)),
            dma((chunks, 5)),
            dma((chunks, ranks)),
            dma((chunks,)),
            dma((chunks,)),
            dma((ranks,)),
            dma((ranks,)),
            dma((2,)),
            dma((2 * STATES + 2 * chunks + 2,)),
        ],
        compiler_params=pltpu.CompilerParams(
            collective_id=0, has_side_effects=True, vmem_limit_bytes=62 * 2**20
        ),
    )(
        failed,
        jnp.broadcast_to(failed.astype(f32)[:, None], (8, 128)),
        document.reshape(blocks, 1, lane_rows),
        document.reshape(blocks, lane_rows, 1),
        acts,
        *states,
    )


def shards_pair(
    failed_section,
    token_ids,
    section_outputs,
    *states,
):
    sections = lax.axis_size("section")
    ranks = lax.axis_size("tensor")
    section = lax.axis_index("section")
    replica = lax.axis_index("dp")
    replacing = section == jnp.remainder(failed_section[0], sections)
    own = [array[0] for array in states]
    half_rows = own[0].shape[0]
    fetched, context, out_rows = relay_call(
        failed_section, document_ids(token_ids[0]), section_outputs[0, 0], own, ranks
    )
    tokens = section_outputs.shape[2]
    context = jnp.transpose(context, (1, 3, 2, 0, 4)).reshape(tokens, -1)
    out_rows = jnp.transpose(out_rows, (2, 1, 0, 3)).reshape(out_rows.shape[2], -1)
    update = lax.dot_general(
        context, out_rows, (((1,), (1,)), ((), ())), preferred_element_type=jnp.float32
    ).astype(jnp.bfloat16)

    def placed(array, other):
        other = jnp.concatenate([other[0], other[1]], axis=1).astype(jnp.float32)
        halves = jnp.stack(
            [jnp.where(replica == half, array, other) for half in range(2)]
        ).reshape(2 * half_rows, -1)
        return jnp.where(replacing, halves, 0.0)[None, None]

    return tuple(placed(array, fetched[j]) for j, array in enumerate(own)) + (
        jnp.where(replacing, update, jnp.zeros_like(update))[None, None],
    )


def solution(mesh):
    paired = tuple(mesh.shape[axis] for axis in ("dp", "section", "tensor")) == (2, 4, 4)
    return jax.shard_map(
        shards_pair if paired else shards,
        mesh=mesh,
        in_specs=(
            P("dp"),
            P("dp", None),
            P("dp", "section", None, "tensor"),
            P("section", "dp", "tensor"),
            P("section", "dp", "tensor"),
            P("section", "dp", "tensor"),
            P("section", "dp", "tensor"),
            P("section", "dp", "tensor"),
            P("section", "dp", "tensor"),
            P("section", "dp", "tensor"),
            P("section", "dp", "tensor"),
        ),
        out_specs=(
            P("dp", "section", None, "tensor"),
            P("dp", "section", None, "tensor"),
            P("dp", "section", None, "tensor"),
            P("dp", "section", None, "tensor"),
            P("dp", "section", None, "tensor"),
            P("dp", "section", None, "tensor"),
            P("dp", "section", None, "tensor"),
            P("dp", "section", None, "tensor"),
            P("dp", "section", None, "tensor"),
        ),
        check_vma=False,
    )
```

```python
import math

import jax
import jax.numpy as jnp
from jax import lax
from jax.experimental import pallas as pl
from jax.experimental.pallas import tpu as pltpu
from jax.sharding import PartitionSpec as P

HD = 128


end_token = 100001
mask_fill = -1e30


def passed_along(array, axis, by):
    count = lax.axis_size(axis)
    return lax.ppermute(array, axis, [(i, (i + by) % count) for i in range(count)])


def document_ids(token_row):
    doc_ends = (token_row == end_token).astype(jnp.int32)
    return jnp.cumsum(doc_ends) - doc_ends


def attend(queries, key_vals, value_vals, token_row):
    token_count = queries.shape[0]
    heads_local = queries.shape[1] // HD
    block_rows = min(512, token_count)
    document = document_ids(token_row)
    positions = jnp.arange(token_count, dtype=jnp.int32)
    key_heads = key_vals.reshape(token_count, heads_local, HD)
    value_heads = value_vals.reshape(token_count, heads_local, HD)

    def one_block(block_index):
        first_row = block_index * block_rows
        query_block = lax.dynamic_slice_in_dim(queries, first_row, block_rows, 0).reshape(
            block_rows, heads_local, HD
        )
        scores = jnp.einsum(
            "qhd,khd->hqk", query_block, key_heads, preferred_element_type=jnp.float32
        ) * (1.0 / math.sqrt(HD))
        query_pos = lax.dynamic_slice_in_dim(positions, first_row, block_rows, 0)
        query_doc = lax.dynamic_slice_in_dim(document, first_row, block_rows, 0)
        allowed = (positions[None, :] <= query_pos[:, None]) & (
            document[None, :] == query_doc[:, None]
        )
        scores = jnp.where(allowed[None], scores, mask_fill)
        highest = jnp.max(scores, axis=2, keepdims=True)
        weights = jnp.exp(scores - highest)
        probs = (weights / jnp.sum(weights, axis=2, keepdims=True)).astype(jnp.bfloat16)
        context = jnp.einsum(
            "hqk,khd->qhd", probs, value_heads, preferred_element_type=jnp.float32
        ).astype(jnp.bfloat16)
        return context.reshape(block_rows, heads_local * HD)

    blocks = lax.map(one_block, jnp.arange(token_count // block_rows, dtype=jnp.int32))
    return blocks.reshape(token_count, heads_local * HD)


def shards(
    failed_section,
    token_ids,
    section_outputs,
    w_query,
    w_key,
    w_value,
    w_out,
    m_value,
    v_value,
    m_out,
    v_out,
):
    section_failed = jnp.remainder(failed_section[0], lax.axis_size("section"))
    replacing = lax.axis_index("section") == section_failed
    states = (
        lax.all_gather(w_query, "dp", axis=1, tiled=True),
        lax.all_gather(w_key, "dp", axis=1, tiled=True),
        lax.all_gather(w_value, "dp", axis=1, tiled=True),
        lax.all_gather(w_out, "dp", axis=1, tiled=True),
        lax.all_gather(m_value, "dp", axis=1, tiled=True),
        lax.all_gather(v_value, "dp", axis=1, tiled=True),
        lax.all_gather(m_out, "dp", axis=1, tiled=True),
        lax.all_gather(v_out, "dp", axis=1, tiled=True),
    )
    masters = states[:4]
    moments = states[4:]
    query_bf = masters[0][0].astype(jnp.bfloat16)
    key_bf = masters[1][0].astype(jnp.bfloat16)
    value_bf = masters[2][0].astype(jnp.bfloat16)
    out_bf = masters[3][0].astype(jnp.bfloat16)
    inner_local = query_bf.shape[1]
    w_joined = jnp.concatenate([query_bf, key_bf, value_bf], axis=1)
    incoming = passed_along(section_outputs, "section", 1)
    projected = jnp.dot(
        lax.all_gather(incoming, "tensor", axis=3, tiled=True)[0, 0],
        w_joined,
        preferred_element_type=jnp.float32,
    )
    queries = projected[:, :inner_local].astype(jnp.bfloat16)
    key_vals = projected[:, inner_local : 2 * inner_local].astype(jnp.bfloat16)
    value_vals = projected[:, 2 * inner_local :].astype(jnp.bfloat16)
    context = attend(queries, key_vals, value_vals, token_ids[0])
    context_whole = lax.all_gather(context, "tensor", axis=1, tiled=True)
    out_slice = lax.all_to_all(out_bf, "tensor", split_axis=0, concat_axis=1, tiled=True)
    update = lax.dot_general(
        context_whole, out_slice, (((1,), (1,)), ((), ())), preferred_element_type=jnp.float32
    ).astype(jnp.bfloat16)

    def placed(gathered):
        return jnp.where(replacing, gathered[None], jnp.zeros_like(gathered[None]))

    update_block = jnp.where(
        replacing, update[None, None], jnp.zeros((1, 1) + update.shape, jnp.bfloat16)
    )
    return (
        placed(masters[0]),
        placed(masters[1]),
        placed(masters[2]),
        placed(masters[3]),
        placed(moments[0]),
        placed(moments[1]),
        placed(moments[2]),
        placed(moments[3]),
        update_block,
    )


MESH = pl.DeviceIdType.MESH
PARTS = ((2, True), (2, True), (2, True), (1, False), (1, False))
STATES = 8


def relay_kernel(
    f_ref,
    ids,
    acts,
    s0,
    s1,
    s2,
    s3,
    s4,
    s5,
    s6,
    s7,
    state_out,
    update_out,
    f_vec,
    f_peer,
    doc_row,
    doc_col,
    own_f32,
    own_bf,
    pair_bf,
    to_peer,
    held,
    x_own,
    x_pair,
    x_mine,
    x_flip,
    x_all,
    qkv,
    qkv_pair,
    ctx,
    out_rows,
    update,
    update_far,
    load_x_sem,
    load_s_sem,
    f_sems,
    pair_x_send,
    pair_x_recv,
    flip_send,
    flip_recv,
    rest_send,
    rest_recv,
    pair_s_send,
    pair_s_recv,
    cross_send,
    cross_recv,
    got_send,
    got_recv,
    line_send,
    line_recv,
    over_send,
    over_recv,
    qkv_send,
    qkv_recv,
    ctx_send,
    ctx_recv,
    ctxp_send,
    ctxp_recv,
    rows_send,
    rows_recv,
    rowsp_sems,
    far_send,
    far_recv,
    updp_send,
    updp_recv,
    out_sems,
):
    states = (s0, s1, s2, s3, s4, s5, s6, s7)
    replica = lax.axis_index("dp")
    section = lax.axis_index("section")
    rank = lax.axis_index("tensor")
    side = section // 2
    core = section % 2
    other_core = 1 - core
    peer = 1 - replica
    pair_id = {"section": side * 2 + other_core}
    flip_id = {"section": (1 - side) * 2 + core}
    peer_id = {"dp": peer}
    sections = 4
    ranks = ctx.shape[1]
    tokens = 2 * x_own.shape[0]
    unit = tokens // (2 * sum(part for part, _ in PARTS))
    chunks = len(PARTS)
    shared = [pair for _, pair in PARTS]
    size = [part * unit for part, _ in PARTS]
    start = [sum(size[:k]) for k in range(chunks)]
    width = x_own.shape[1]
    half_rows = held.shape[3]
    block_width = update.shape[2]
    middle = (rank == 1) | (rank == 2)
    scale = math.log2(math.e) / math.sqrt(HD)

    def remote(src, dst, send, recv, where_to):
        return pltpu.make_async_remote_copy(
            src_ref=src,
            dst_ref=dst,
            send_sem=send,
            recv_sem=recv,
            device_id=where_to,
            device_id_type=MESH,
        )

    def lane_rows(k):
        return pl.ds(start[k], size[k])

    def chunk_rows(k):
        return pl.ds(2 * start[k], 2 * size[k])

    def token_rows(k, lane):
        return pl.ds(pl.multiple_of(2 * start[k] + lane * size[k], unit), size[k])

    def side_rows(k, which):
        if not shared[k]:
            return lane_rows(k)
        half = size[k] // 2
        return pl.ds(pl.multiple_of(start[k] + which * half, half), half)

    def mine_rows(k):
        return side_rows(k, side)

    def flip_rows(k):
        return side_rows(k, 1 - side)

    def load_x(k):
        return pltpu.make_async_copy(
            acts.at[token_rows(k, core)], x_own.at[lane_rows(k)], load_x_sem.at[k]
        )

    def load_s(j):
        return pltpu.make_async_copy(states[j], own_f32.at[j], load_s_sem.at[j])

    def pair_x(k):
        return remote(
            acts.at[token_rows(k, other_core)],
            x_pair.at[lane_rows(k)],
            pair_x_send.at[k],
            pair_x_recv.at[k],
            pair_id,
        )

    def f_copy():
        return remote(f_vec, f_peer, f_sems.at[0], f_sems.at[1], peer_id)

    def flip_x(k, rows):
        return remote(
            x_mine.at[rows], x_flip.at[rows], flip_send.at[k], flip_recv.at[k], flip_id
        )

    def rest_x(k, rows):
        return remote(
            x_mine.at[rows], x_flip.at[rows], rest_send.at[k], rest_recv.at[k], flip_id
        )

    def pair_s(j):
        if j < 3:
            return remote(
                own_bf.at[j], pair_bf.at[j], pair_s_send.at[j], pair_s_recv.at[j], pair_id
            )
        return remote(
            own_bf.at[j, other_core],
            pair_bf.at[j, other_core],
            pair_s_send.at[j],
            pair_s_recv.at[j],
            pair_id,
        )

    def pair_s_arrival(j):
        if j < 3:
            return pair_s(j)
        return remote(
            own_bf.at[j, core],
            pair_bf.at[j, core],
            pair_s_send.at[j],
            pair_s_recv.at[j],
            pair_id,
        )

    def cross(j):
        return remote(
            to_peer.at[j], held.at[replica, j, core], cross_send.at[j], cross_recv.at[j], peer_id
        )

    def cross_arrival(j):
        return remote(
            to_peer.at[j], held.at[peer, j, core], cross_send.at[j], cross_recv.at[j], peer_id
        )

    def got(j):
        return remote(
            held.at[peer, j, core],
            held.at[peer, j, core],
            got_send.at[j],
            got_recv.at[j],
            pair_id,
        )

    def got_arrival(j):
        return remote(
            held.at[peer, j, other_core],
            held.at[peer, j, other_core],
            got_send.at[j],
            got_recv.at[j],
            pair_id,
        )

    def line(k, owner, slot, target):
        part = x_all.at[owner, mine_rows(k)]
        return remote(
            part, part, line_send.at[k, slot], line_recv.at[k, owner], {"tensor": target}
        )

    def over(k, owner):
        part = x_all.at[owner, mine_rows(k)]
        return remote(part, part, over_send.at[k, owner], over_recv.at[k, owner], flip_id)

    def over_arrival(k, owner):
        part = x_all.at[owner, flip_rows(k)]
        return remote(part, part, over_send.at[k, owner], over_recv.at[k, owner], flip_id)

    def qkv_copy(k, lane):
        return remote(
            qkv_pair.at[:, lane_rows(k)],
            qkv.at[:, token_rows(k, lane)],
            qkv_send.at[k],
            qkv_recv.at[k],
            pair_id,
        )

    def ctx_line(k, owner, slot, target):
        part = ctx.at[core, owner, chunk_rows(k)]
        return remote(
            part, part, ctx_send.at[k, slot], ctx_recv.at[k, owner], {"tensor": target}
        )

    def ctx_pair_copy(k, lane):
        part = ctx.at[lane, :, chunk_rows(k)]
        return remote(part, part, ctxp_send.at[k], ctxp_recv.at[k], pair_id)

    def rows_copy(target):
        return remote(
            held.at[target - 1, 3, core],
            out_rows.at[core, rank],
            rows_send.at[target],
            rows_recv.at[rank],
            {"tensor": target},
        )

    def rows_arrival(owner):
        part = out_rows.at[core, owner]
        return remote(
            part, part, rows_send.at[1], rows_recv.at[owner], {"tensor": owner}
        )

    def rows_pair_copy(lane):
        part = out_rows.at[lane]
        return remote(part, part, rowsp_sems.at[0], rowsp_sems.at[1], pair_id)

    end_rank = jnp.where(rank == 1, 0, ranks - 1)

    def far_copy(k):
        return remote(
            update_far.at[chunk_rows(k)],
            update.at[core, chunk_rows(k)],
            far_send.at[k],
            far_recv.at[k],
            {"tensor": end_rank},
        )

    def far_arrival(k):
        part = update.at[core, chunk_rows(k)]
        near_rank = jnp.where(rank == 0, 1, 2)
        return remote(
            part, part, far_send.at[k], far_recv.at[k], {"tensor": near_rank}
        )

    def update_pair_copy(k, lane):
        part = update.at[lane, chunk_rows(k)]
        return remote(part, part, updp_send.at[k], updp_recv.at[k], pair_id)

    def update_out_copy(k, lane, sem):
        return pltpu.make_async_copy(
            update.at[lane, chunk_rows(k)], update_out.at[lane, chunk_rows(k)], sem
        )

    def at_ranks(*places):
        def run(body):
            for where_at, slot, target in places:

                @pl.when(rank == where_at)
                def _(slot=slot, target=target):
                    body(slot, target)

        return run

    near = at_ranks(
        (1, 1, 0),
        (1, 0, 2),
        (2, 1, 3),
        (2, 0, 1),
        (0, 0, 1),
        (0, 1, 2),
        (3, 0, 2),
        (3, 1, 1),
    )
    to_middle = at_ranks(
        (0, 1, 2),
        (0, 0, 1),
        (3, 1, 1),
        (3, 0, 2),
        (1, 0, 2),
        (2, 0, 1),
    )

    def arrivals_at(step, body):
        for sign in (1, -1):
            owner = rank - sign * step

            @pl.when((owner >= 0) & (owner < ranks))
            def _(owner=owner):
                body(owner)

    def arrivals(body):
        for step in (1, 2, 3):
            arrivals_at(step, body)

    def relayed(step, body):
        @pl.when(rank == 2)
        def _():
            body(2 - step, 1 + step, 3)

        @pl.when(rank == 1)
        def _():
            body(1 + step, 1 + step, 0)

    f_mine = lax.rem(f_ref[0], sections)
    f_from = lax.rem(f_mine + sections - 1, sections)
    from_core = lax.rem(f_from, 2) == core
    from_side = (f_from // 2) == side
    f_core = lax.rem(f_mine, 2) == core

    for k in range(chunks):
        load_x(k).start()
    for j in range(STATES):
        load_s(j).start()

    barrier = pltpu.get_barrier_semaphore()
    for where_to in (pair_id, flip_id, peer_id):
        pl.semaphore_signal(barrier, inc=1, device_id=where_to, device_id_type=MESH)
    for step in range(1, ranks):
        pl.semaphore_signal(
            barrier,
            inc=1,
            device_id={"tensor": lax.rem(rank + step, ranks)},
            device_id_type=MESH,
        )
    pl.semaphore_wait(barrier, 2 + ranks)

    f_vec[...] = jnp.full(f_vec.shape, f_mine).astype(jnp.float32)
    f_copy().start()
    for k in range(chunks):
        pair_x(k).start()

    def spread(k):
        load_x(k).wait()
        pair_x(k).wait_recv()
        rows = lane_rows(k)
        x_mine[rows] = jnp.where(from_core, x_own[rows], x_pair[rows])
        flip_x(k, flip_rows(k)).start()

    def settle(k):
        rows = mine_rows(k)
        flip_x(k, rows).wait_recv()
        x_all[rank, rows] = jnp.where(from_side, x_mine[rows], x_flip[rows])
        near(lambda slot, target: line(k, rank, slot, target).start())

    def rest(k):
        if shared[k]:
            rest_x(k, mine_rows(k)).start()

    def settle_rest(k):
        if shared[k]:
            rows = flip_rows(k)
            rest_x(k, rows).wait_recv()
            x_all[rank, rows] = jnp.where(from_side, x_mine[rows], x_flip[rows])

    def forward(k):
        def one(owner):
            line(k, owner, 0, owner).wait_recv()
            if shared[k]:
                over(k, owner).start()

        def steps():
            for step in (1, 2, 3):
                arrivals_at(step, one)
                if step < 3:
                    relayed(
                        step, lambda owner, slot, target: line(k, owner, slot, target).start()
                    )

        if shared[k]:
            steps()
        else:
            pl.when(middle)(steps)

    def documents():
        lanes = 128
        shape = (lanes, lanes)
        before = lax.broadcasted_iota(jnp.int32, shape, 0)
        after = lax.broadcasted_iota(jnp.int32, shape, 1)
        upper = jnp.where(before < after, 1.0, 0.0).astype(jnp.bfloat16)
        lower = jnp.where(after < before, 1.0, 0.0).astype(jnp.bfloat16)
        count = jnp.zeros((1, 1), jnp.float32)
        for first in range(0, tokens, lanes):
            found = jnp.where(ids[:, first : first + lanes] == end_token, 1.0, 0.0)
            ends = jnp.broadcast_to(found, (8, lanes)).astype(jnp.bfloat16)
            row = jnp.dot(ends, upper, preferred_element_type=jnp.float32)
            column = lax.dot_general(
                lower, ends, (((1,), (1,)), ((), ())), preferred_element_type=jnp.float32
            )
            doc_row[:, first : first + lanes] = row[:1] + count
            doc_col[first : first + lanes] = column[:, :1] + count
            count = count + jnp.sum(found, axis=1, keepdims=True)

    def rounded(j):
        load_s(j).wait()

        @pl.loop(0, half_rows // 128)
        def _(i):
            rows = pl.ds(pl.multiple_of(i * 128, 128), 128)
            own_bf[j, 0, rows] = own_f32[j, rows, :HD].astype(jnp.bfloat16)
            own_bf[j, 1, rows] = own_f32[j, rows, HD:].astype(jnp.bfloat16)

        pair_s(j).start()

    def chosen(j, peer_core):
        pair_s_arrival(j).wait_recv()
        to_peer[j] = jnp.where(peer_core, own_bf[j, core], pair_bf[j, core])
        cross(j).start()
        if j < 3:
            held[replica, j] = jnp.where(f_core, own_bf[j], pair_bf[j])
        if j == 3:
            held[replica, j, core] = jnp.where(f_core, own_bf[j, core], pair_bf[j, core])

    def state_out_copy(j, lane, sem):
        return pltpu.make_async_copy(held.at[peer, j, lane], state_out.at[j, lane], sem)

    def arrived(j):
        cross_arrival(j).wait_recv()
        got(j).start()
        state_out_copy(j, core, out_sems.at[j]).start()

    def paired(j):
        got_arrival(j).wait_recv()
        state_out_copy(j, other_core, out_sems.at[STATES + j]).start()

    def project(k):
        if shared[k]:
            settle_rest(k)
            arrivals(lambda owner: over_arrival(k, owner).wait_recv())
        else:

            @pl.when(jnp.logical_not(middle))
            def _():
                arrivals(lambda owner: line(k, owner, 0, owner).wait_recv())

        total = None
        per_half = half_rows // width
        for b in range(ranks):
            half, rows = b // per_half, pl.ds((b % per_half) * width, width)
            weight = jnp.concatenate(
                [held[half, j, lane, rows] for j in range(3) for lane in range(2)], axis=1
            )
            part = jnp.dot(x_all[b, lane_rows(k)], weight, preferred_element_type=jnp.float32)
            total = part if total is None else total + part
        for j in range(3):
            first = total[:, (2 * j) * HD : (2 * j + 1) * HD].astype(jnp.bfloat16)
            second = total[:, (2 * j + 1) * HD : (2 * j + 2) * HD].astype(jnp.bfloat16)
            qkv[j, token_rows(k, core)] = jnp.where(core == 0, first, second)
            qkv_pair[j, lane_rows(k)] = jnp.where(core == 0, second, first)
        qkv_copy(k, core).start()

    def attend_rows(k, lane):
        dims = (((1,), (1,)), ((), ()))
        first = 2 * start[k] + lane * size[k]
        last = first + size[k]
        q = qkv[0, first:last]
        docs = doc_col[first:last]
        shape = (size[k], size[k])
        parts = []
        if first > 0:
            s = lax.dot_general(q, qkv[1, :first], dims, preferred_element_type=jnp.float32)
            parts.append(jnp.where(doc_row[:, :first] == docs, s, mask_fill))
        s = lax.dot_general(q, qkv[1, first:last], dims, preferred_element_type=jnp.float32)
        allowed = (doc_row[:, first:last] == docs) & (
            lax.broadcasted_iota(jnp.int32, shape, 1)
            <= lax.broadcasted_iota(jnp.int32, shape, 0)
        )
        parts.append(jnp.where(allowed, s, mask_fill))
        s = jnp.concatenate(parts, axis=1)
        high = jnp.max(s, axis=1, keepdims=True)
        weights = jnp.exp2((s - high) * scale)
        total = jnp.sum(weights, axis=1, keepdims=True)
        acc = jnp.dot(
            weights.astype(jnp.bfloat16), qkv[2, :last], preferred_element_type=jnp.float32
        )
        ctx[core, rank, first:last] = (acc / total).astype(jnp.bfloat16)

    def attend(k):
        qkv_copy(k, other_core).wait_recv()
        for lane in range(2):
            attend_rows(k, lane)
        to_middle(lambda slot, target: ctx_line(k, rank, slot, target).start())

    def collect(k):
        @pl.when(middle)
        def _():
            arrivals(lambda owner: ctx_line(k, owner, 0, owner).wait_recv())
            ctx_pair_copy(k, core).start()

    def send_rows(local):
        for target in (1, 2):
            held_here = replica == target - 1
            ready = held_here if local else jnp.logical_not(held_here)

            @pl.when(ready & (rank != target))
            def _(target=target):
                rows_copy(target).start()

            @pl.when(ready & (rank == target))
            def _(target=target):
                out_rows[core, target] = held[target - 1, 3, core]

    def take_rows():
        @pl.when(middle)
        def _():
            arrivals(lambda owner: rows_arrival(owner).wait_recv())
            rows_pair_copy(core).start()

    def take_rows_pair():
        @pl.when(middle)
        def _():
            rows_pair_copy(other_core).wait_recv()

    heads = [(b, lane) for b in range(ranks) for lane in range(2)]
    block_rows = half_rows // 2

    def project_out(k):
        @pl.when(middle)
        def _():
            ctx_pair_copy(k, other_core).wait_recv()
            left = jnp.concatenate([ctx[lane, b, chunk_rows(k)] for b, lane in heads], axis=1)

            def block(first):
                rows = pl.ds(
                    pl.multiple_of(first + core * block_width, block_width), block_width
                )
                right = jnp.concatenate([out_rows[lane, b, rows] for b, lane in heads], axis=1)
                return lax.dot_general(
                    left, right, (((1,), (1,)), ((), ())), preferred_element_type=jnp.float32
                ).astype(jnp.bfloat16)

            update_far[chunk_rows(k)] = block(jnp.where(rank == 1, 0, block_rows))
            far_copy(k).start()
            update[core, chunk_rows(k)] = block(jnp.where(rank == 1, block_rows, 0))
            update_pair_copy(k, core).start()
            update_out_copy(k, core, out_sems.at[2 * STATES + k]).start()

    def take_update(k):
        @pl.when(jnp.logical_not(middle))
        def _():
            far_arrival(k).wait_recv()
            update_pair_copy(k, core).start()
            update_out_copy(k, core, out_sems.at[2 * STATES + k]).start()

    def take_update_pair(k):
        update_pair_copy(k, other_core).wait_recv()
        update_out_copy(k, other_core, out_sems.at[2 * STATES + chunks + k]).start()

    spread(0)
    spread(1)
    for j in range(4):
        rounded(j)
    for k in range(2, chunks):
        spread(k)
    f_copy().wait_recv()
    peer_core = lax.rem(jnp.max(f_peer[...]).astype(jnp.int32), 2) == core
    settle(0)
    for j in range(4):
        chosen(j, peer_core)
    settle(1)
    rest(0)
    for j in range(4, STATES):
        rounded(j)
    settle(2)
    rest(1)
    forward(0)
    for j in range(4, STATES):
        chosen(j, peer_core)
    settle(3)
    send_rows(True)
    rest(2)
    documents()
    forward(1)
    settle(4)
    for j in range(3):
        arrived(j)
    forward(2)
    for j in range(3):
        paired(j)
    project(0)
    arrived(3)
    send_rows(False)
    attend(0)
    forward(3)
    project(1)
    attend(1)
    forward(4)
    project(2)
    attend(2)
    take_rows()
    collect(0)
    project(3)
    attend(3)
    take_rows_pair()
    project_out(0)
    collect(1)
    project(4)
    attend(4)
    project_out(1)
    collect(2)
    take_update(0)
    project_out(2)
    take_update(1)
    collect(3)
    take_update_pair(0)
    for j in range(4, STATES):
        arrived(j)
    project_out(3)
    take_update(2)
    take_update_pair(1)
    collect(4)
    for j in range(3, STATES):
        paired(j)
    project_out(4)
    take_update_pair(2)
    take_update(3)
    take_update_pair(3)
    take_update(4)
    take_update_pair(4)

    f_copy().wait_send()
    for k in range(chunks):
        pair_x(k).wait_send()
        flip_x(k, flip_rows(k)).wait_send()
        near(lambda slot, target: line(k, rank, slot, target).wait_send())
        for step in (1, 2):
            relayed(
                step, lambda owner, slot, target: line(k, owner, slot, target).wait_send()
            )
        if shared[k]:
            rest_x(k, mine_rows(k)).wait_send()
            arrivals(lambda owner: over(k, owner).wait_send())
        qkv_copy(k, core).wait_send()
        to_middle(lambda slot, target: ctx_line(k, rank, slot, target).wait_send())

        @pl.when(middle)
        def _(k=k):
            ctx_pair_copy(k, core).wait_send()
            far_copy(k).wait_send()

        update_pair_copy(k, core).wait_send()
        update_out_copy(k, core, out_sems.at[2 * STATES + k]).wait()
        update_out_copy(k, other_core, out_sems.at[2 * STATES + chunks + k]).wait()
    for j in range(STATES):
        pair_s(j).wait_send()
        cross(j).wait_send()
        got(j).wait_send()
        state_out_copy(j, core, out_sems.at[j]).wait()
        state_out_copy(j, other_core, out_sems.at[STATES + j]).wait()
    for target in (1, 2):

        @pl.when(rank != target)
        def _(target=target):
            rows_copy(target).wait_send()

    @pl.when(middle)
    def _():
        rows_pair_copy(core).wait_send()


def relay_call(failed, ids, acts, states, ranks):
    tokens, width = acts.shape
    half_rows, inner_local = states[0].shape
    chunks = len(PARTS)
    lane_tokens = tokens // 2
    out_width = 2 * half_rows // ranks
    bf, f32 = jnp.bfloat16, jnp.float32
    vmem, dma = pltpu.VMEM, pltpu.SemaphoreType.DMA
    anywhere = pl.BlockSpec(memory_space=pl.ANY)
    in_vmem = pl.BlockSpec(memory_space=pltpu.VMEM)
    return pl.pallas_call(
        relay_kernel,
        out_shape=(
            jax.ShapeDtypeStruct((STATES, 2, half_rows, HD), bf),
            jax.ShapeDtypeStruct((2, tokens, out_width // 2), bf),
        ),
        in_specs=[pl.BlockSpec(memory_space=pltpu.SMEM), in_vmem]
        + [anywhere] * (1 + STATES),
        out_specs=(anywhere,) * 2,
        scratch_shapes=[
            vmem((8, 128), f32),
            vmem((8, 128), f32),
            vmem((1, tokens), f32),
            vmem((tokens, 1), f32),
            vmem((STATES, half_rows, inner_local), f32),
            vmem((STATES, 2, half_rows, HD), bf),
            vmem((STATES, 2, half_rows, HD), bf),
            vmem((STATES, half_rows, HD), bf),
            vmem((2, STATES, 2, half_rows, HD), bf),
            vmem((lane_tokens, width), bf),
            vmem((lane_tokens, width), bf),
            vmem((lane_tokens, width), bf),
            vmem((lane_tokens, width), bf),
            vmem((ranks, lane_tokens, width), bf),
            vmem((3, tokens, HD), bf),
            vmem((3, lane_tokens, HD), bf),
            vmem((2, ranks, tokens, HD), bf),
            vmem((2, ranks, half_rows, HD), bf),
            vmem((2, tokens, out_width // 2), bf),
            vmem((tokens, out_width // 2), bf),
            dma((chunks,)),
            dma((STATES,)),
            dma((2,)),
            dma((chunks,)),
            dma((chunks,)),
            dma((chunks,)),
            dma((chunks,)),
            dma((chunks,)),
            dma((chunks,)),
            dma((STATES,)),
            dma((STATES,)),
            dma((STATES,)),
            dma((STATES,)),
            dma((STATES,)),
            dma((STATES,)),
            dma((chunks, ranks)),
            dma((chunks, ranks)),
            dma((chunks, ranks)),
            dma((chunks, ranks)),
            dma((chunks,)),
            dma((chunks,)),
            dma((chunks, 2)),
            dma((chunks, ranks)),
            dma((chunks,)),
            dma((chunks,)),
            dma((ranks,)),
            dma((ranks,)),
            dma((2,)),
            dma((chunks,)),
            dma((chunks,)),
            dma((chunks,)),
            dma((chunks,)),
            dma((2 * STATES + 2 * chunks,)),
        ],
        compiler_params=pltpu.CompilerParams(
            collective_id=0, has_side_effects=True, vmem_limit_bytes=62 * 2**20
        ),
    )(
        failed,
        ids,
        acts,
        *states,
    )


def finish_kernel(
    place,
    s0,
    s1,
    s2,
    s3,
    s4,
    s5,
    s6,
    s7,
    fetched,
    update_halves,
    o0,
    o1,
    o2,
    o3,
    o4,
    o5,
    o6,
    o7,
    update_out,
    own,
    other,
    wide,
    halves,
    update,
    own_sems,
    other_sems,
    own_out_sems,
    wide_sems,
    halves_sems,
    update_sems,
):
    states = (s0, s1, s2, s3, s4, s5, s6, s7)
    outs = (o0, o1, o2, o3, o4, o5, o6, o7)
    replica = place[0]
    keep = place[1] == 1
    half_rows = own.shape[1]
    chunks, chunk_rows = update.shape[:2]
    half_width = halves.shape[2]
    own_rows = pl.ds(pl.multiple_of(replica * half_rows, half_rows), half_rows)
    other_rows = pl.ds(pl.multiple_of((1 - replica) * half_rows, half_rows), half_rows)
    slots = wide.shape[0]
    step_rows = 64

    def load_own(j):
        return pltpu.make_async_copy(states[j], own.at[j], own_sems.at[j])

    def load_other(j):
        return pltpu.make_async_copy(fetched.at[j], other.at[j], other_sems.at[j])

    def load_halves(k):
        rows = pl.ds(k * chunk_rows, chunk_rows)
        return pltpu.make_async_copy(
            update_halves.at[:, rows], halves.at[:, rows], halves_sems.at[k]
        )

    def store_own(j):
        return pltpu.make_async_copy(own.at[j], outs[j].at[own_rows], own_out_sems.at[j])

    def store_other(j):
        return pltpu.make_async_copy(
            wide.at[j % slots], outs[j].at[other_rows], wide_sems.at[j % slots]
        )

    def store_update(k):
        return pltpu.make_async_copy(
            update.at[k], update_out.at[pl.ds(k * chunk_rows, chunk_rows)], update_sems.at[k]
        )

    for j in range(STATES):
        load_own(j).start()
        load_other(j).start()
        if j < chunks:
            load_halves(j).start()

    def one_update(k):
        load_halves(k).wait()
        rows = pl.ds(k * chunk_rows, chunk_rows)
        for half in range(2):
            update[k, :, half * half_width : (half + 1) * half_width] = jnp.where(
                keep, halves[half, rows], jnp.zeros((chunk_rows, half_width), update.dtype)
            )
        store_update(k).start()

    for j in range(STATES):
        load_own(j).wait()

        @pl.loop(0, half_rows // step_rows)
        def _(i):
            part = pl.ds(pl.multiple_of(i * step_rows, step_rows), step_rows)
            own[j, part] = jnp.where(keep, own[j, part], 0.0)

        store_own(j).start()
        load_other(j).wait()
        if j >= slots:
            store_other(j - slots).wait()

        @pl.loop(0, half_rows // step_rows)
        def _(i):
            part = pl.ds(pl.multiple_of(i * step_rows, step_rows), step_rows)
            for lane in range(2):
                wide[j % slots, part, lane * HD : (lane + 1) * HD] = jnp.where(
                    keep, other[j, lane, part].astype(jnp.float32), 0.0
                )

        store_other(j).start()
        if j < chunks:
            one_update(j)

    for j in range(STATES - slots, STATES):
        store_other(j).wait()
    for j in range(STATES):
        store_own(j).wait()
    for k in range(chunks):
        store_update(k).wait()


def finish_call(place, own, fetched, update_halves):
    half_rows, inner_local = own[0].shape
    _, tokens, half_width = update_halves.shape
    chunks = 4
    chunk_rows = tokens // chunks
    out_width = 2 * half_width
    bf, f32 = jnp.bfloat16, jnp.float32
    vmem, dma = pltpu.VMEM, pltpu.SemaphoreType.DMA
    anywhere = pl.BlockSpec(memory_space=pl.ANY)
    slots = 4
    return pl.pallas_call(
        finish_kernel,
        out_shape=[jax.ShapeDtypeStruct((2 * half_rows, inner_local), f32)] * STATES
        + [jax.ShapeDtypeStruct((chunks * chunk_rows, out_width), bf)],
        in_specs=[pl.BlockSpec(memory_space=pltpu.SMEM)] + [anywhere] * (STATES + 2),
        out_specs=[anywhere] * (STATES + 1),
        scratch_shapes=[
            vmem((STATES, half_rows, inner_local), f32),
            vmem(fetched.shape, bf),
            vmem((slots, half_rows, inner_local), f32),
            vmem(update_halves.shape, bf),
            vmem((chunks, chunk_rows, out_width), bf),
            dma((STATES,)),
            dma((STATES,)),
            dma((STATES,)),
            dma((slots,)),
            dma((chunks,)),
            dma((chunks,)),
        ],
        compiler_params=pltpu.CompilerParams(vmem_limit_bytes=62 * 2**20),
    )(place, *own, fetched, update_halves)


def shards_pair(
    failed_section,
    token_ids,
    section_outputs,
    *states,
):
    sections = lax.axis_size("section")
    ranks = lax.axis_size("tensor")
    section = lax.axis_index("section")
    replica = lax.axis_index("dp")
    replacing = section == jnp.remainder(failed_section[0], sections)
    own = [array[0] for array in states]
    fetched, update_halves = relay_call(
        failed_section, token_ids, section_outputs[0, 0], own, ranks
    )
    place = jnp.stack([replica.astype(jnp.int32), replacing.astype(jnp.int32)])
    outs = finish_call(place, own, fetched, update_halves)
    return tuple(out[None, None] for out in outs)


def solution(mesh):
    paired = tuple(mesh.shape[axis] for axis in ("dp", "section", "tensor")) == (2, 4, 4)
    return jax.shard_map(
        shards_pair if paired else shards,
        mesh=mesh,
        in_specs=(
            P("dp"),
            P("dp", None),
            P("dp", "section", None, "tensor"),
            P("section", "dp", "tensor"),
            P("section", "dp", "tensor"),
            P("section", "dp", "tensor"),
            P("section", "dp", "tensor"),
            P("section", "dp", "tensor"),
            P("section", "dp", "tensor"),
            P("section", "dp", "tensor"),
            P("section", "dp", "tensor"),
        ),
        out_specs=(
            P("dp", "section", None, "tensor"),
            P("dp", "section", None, "tensor"),
            P("dp", "section", None, "tensor"),
            P("dp", "section", None, "tensor"),
            P("dp", "section", None, "tensor"),
            P("dp", "section", None, "tensor"),
            P("dp", "section", None, "tensor"),
            P("dp", "section", None, "tensor"),
            P("dp", "section", None, "tensor"),
        ),
        check_vma=False,
    )
```

```python
import math

import jax
import jax.numpy as jnp
from jax import lax
from jax.experimental import pallas as pl
from jax.experimental.pallas import tpu as pltpu
from jax.sharding import PartitionSpec as P

HD = 128


end_token = 100001
mask_fill = -1e30


def passed_along(array, axis, by):
    count = lax.axis_size(axis)
    return lax.ppermute(array, axis, [(i, (i + by) % count) for i in range(count)])


def document_ids(token_row):
    doc_ends = (token_row == end_token).astype(jnp.int32)
    return jnp.cumsum(doc_ends) - doc_ends


def attend(queries, key_vals, value_vals, token_row):
    token_count = queries.shape[0]
    heads_local = queries.shape[1] // HD
    block_rows = min(512, token_count)
    document = document_ids(token_row)
    positions = jnp.arange(token_count, dtype=jnp.int32)
    key_heads = key_vals.reshape(token_count, heads_local, HD)
    value_heads = value_vals.reshape(token_count, heads_local, HD)

    def one_block(block_index):
        first_row = block_index * block_rows
        query_block = lax.dynamic_slice_in_dim(queries, first_row, block_rows, 0).reshape(
            block_rows, heads_local, HD
        )
        scores = jnp.einsum(
            "qhd,khd->hqk", query_block, key_heads, preferred_element_type=jnp.float32
        ) * (1.0 / math.sqrt(HD))
        query_pos = lax.dynamic_slice_in_dim(positions, first_row, block_rows, 0)
        query_doc = lax.dynamic_slice_in_dim(document, first_row, block_rows, 0)
        allowed = (positions[None, :] <= query_pos[:, None]) & (
            document[None, :] == query_doc[:, None]
        )
        scores = jnp.where(allowed[None], scores, mask_fill)
        highest = jnp.max(scores, axis=2, keepdims=True)
        weights = jnp.exp(scores - highest)
        probs = (weights / jnp.sum(weights, axis=2, keepdims=True)).astype(jnp.bfloat16)
        context = jnp.einsum(
            "hqk,khd->qhd", probs, value_heads, preferred_element_type=jnp.float32
        ).astype(jnp.bfloat16)
        return context.reshape(block_rows, heads_local * HD)

    blocks = lax.map(one_block, jnp.arange(token_count // block_rows, dtype=jnp.int32))
    return blocks.reshape(token_count, heads_local * HD)


def shards(
    failed_section,
    token_ids,
    section_outputs,
    w_query,
    w_key,
    w_value,
    w_out,
    m_value,
    v_value,
    m_out,
    v_out,
):
    section_failed = jnp.remainder(failed_section[0], lax.axis_size("section"))
    replacing = lax.axis_index("section") == section_failed
    states = (
        lax.all_gather(w_query, "dp", axis=1, tiled=True),
        lax.all_gather(w_key, "dp", axis=1, tiled=True),
        lax.all_gather(w_value, "dp", axis=1, tiled=True),
        lax.all_gather(w_out, "dp", axis=1, tiled=True),
        lax.all_gather(m_value, "dp", axis=1, tiled=True),
        lax.all_gather(v_value, "dp", axis=1, tiled=True),
        lax.all_gather(m_out, "dp", axis=1, tiled=True),
        lax.all_gather(v_out, "dp", axis=1, tiled=True),
    )
    masters = states[:4]
    moments = states[4:]
    query_bf = masters[0][0].astype(jnp.bfloat16)
    key_bf = masters[1][0].astype(jnp.bfloat16)
    value_bf = masters[2][0].astype(jnp.bfloat16)
    out_bf = masters[3][0].astype(jnp.bfloat16)
    inner_local = query_bf.shape[1]
    w_joined = jnp.concatenate([query_bf, key_bf, value_bf], axis=1)
    incoming = passed_along(section_outputs, "section", 1)
    projected = jnp.dot(
        lax.all_gather(incoming, "tensor", axis=3, tiled=True)[0, 0],
        w_joined,
        preferred_element_type=jnp.float32,
    )
    queries = projected[:, :inner_local].astype(jnp.bfloat16)
    key_vals = projected[:, inner_local : 2 * inner_local].astype(jnp.bfloat16)
    value_vals = projected[:, 2 * inner_local :].astype(jnp.bfloat16)
    context = attend(queries, key_vals, value_vals, token_ids[0])
    context_whole = lax.all_gather(context, "tensor", axis=1, tiled=True)
    out_slice = lax.all_to_all(out_bf, "tensor", split_axis=0, concat_axis=1, tiled=True)
    update = lax.dot_general(
        context_whole, out_slice, (((1,), (1,)), ((), ())), preferred_element_type=jnp.float32
    ).astype(jnp.bfloat16)

    def placed(gathered):
        return jnp.where(replacing, gathered[None], jnp.zeros_like(gathered[None]))

    update_block = jnp.where(
        replacing, update[None, None], jnp.zeros((1, 1) + update.shape, jnp.bfloat16)
    )
    return (
        placed(masters[0]),
        placed(masters[1]),
        placed(masters[2]),
        placed(masters[3]),
        placed(moments[0]),
        placed(moments[1]),
        placed(moments[2]),
        placed(moments[3]),
        update_block,
    )


MESH = pl.DeviceIdType.MESH
PARTS = ((2, True), (2, True), (1, True), (2, True), (1, False))
STATES = 8


def relay_kernel(
    f_ref,
    ids,
    acts,
    s0,
    s1,
    s2,
    s3,
    s4,
    s5,
    s6,
    s7,
    state_out,
    update_out,
    f_vec,
    f_peer,
    doc_row,
    doc_col,
    own_f32,
    own_bf,
    pair_bf,
    to_peer,
    held,
    x_own,
    x_pair,
    x_mine,
    x_flip,
    x_all,
    qkv,
    qkv_pair,
    ctx,
    out_rows,
    update,
    update_far,
    load_x_sem,
    load_s_sem,
    f_sems,
    pair_x_send,
    pair_x_recv,
    flip_send,
    flip_recv,
    rest_send,
    rest_recv,
    pair_s_send,
    pair_s_recv,
    cross_send,
    cross_recv,
    got_send,
    got_recv,
    line_send,
    line_recv,
    over_send,
    over_recv,
    qkv_send,
    qkv_recv,
    ctx_send,
    ctx_recv,
    ctxp_send,
    ctxp_recv,
    rows_send,
    rows_recv,
    rowsp_sems,
    far_send,
    far_recv,
    updp_send,
    updp_recv,
    out_sems,
):
    states = (s0, s1, s2, s3, s4, s5, s6, s7)
    replica = lax.axis_index("dp")
    section = lax.axis_index("section")
    rank = lax.axis_index("tensor")
    side = section // 2
    core = section % 2
    other_core = 1 - core
    peer = 1 - replica
    pair_id = {"section": side * 2 + other_core}
    flip_id = {"section": (1 - side) * 2 + core}
    peer_id = {"dp": peer}
    sections = 4
    ranks = ctx.shape[1]
    tokens = 2 * x_own.shape[0]
    unit = tokens // (2 * sum(part for part, _ in PARTS))
    chunks = len(PARTS)
    shared = [pair for _, pair in PARTS]
    size = [part * unit for part, _ in PARTS]
    start = [sum(size[:k]) for k in range(chunks)]
    width = x_own.shape[1]
    half_rows = held.shape[3]
    block_width = update.shape[2]
    middle = (rank == 1) | (rank == 2)
    scale = math.log2(math.e) / math.sqrt(HD)

    def remote(src, dst, send, recv, where_to):
        return pltpu.make_async_remote_copy(
            src_ref=src,
            dst_ref=dst,
            send_sem=send,
            recv_sem=recv,
            device_id=where_to,
            device_id_type=MESH,
        )

    def lane_rows(k):
        return pl.ds(start[k], size[k])

    def chunk_rows(k):
        return pl.ds(2 * start[k], 2 * size[k])

    def token_rows(k, lane):
        return pl.ds(pl.multiple_of(2 * start[k] + lane * size[k], unit), size[k])

    def side_rows(k, which):
        if not shared[k]:
            return lane_rows(k)
        half = size[k] // 2
        return pl.ds(pl.multiple_of(start[k] + which * half, half), half)

    def mine_rows(k):
        return side_rows(k, side)

    def flip_rows(k):
        return side_rows(k, 1 - side)

    def load_x(k):
        return pltpu.make_async_copy(
            acts.at[token_rows(k, core)], x_own.at[lane_rows(k)], load_x_sem.at[k]
        )

    def load_s(j):
        return pltpu.make_async_copy(states[j], own_f32.at[j], load_s_sem.at[j])

    def pair_x(k):
        return remote(
            acts.at[token_rows(k, other_core)],
            x_pair.at[lane_rows(k)],
            pair_x_send.at[k],
            pair_x_recv.at[k],
            pair_id,
        )

    def f_copy():
        return remote(f_vec, f_peer, f_sems.at[0], f_sems.at[1], peer_id)

    def flip_x(k, rows):
        return remote(
            x_mine.at[rows], x_flip.at[rows], flip_send.at[k], flip_recv.at[k], flip_id
        )

    def rest_x(k, rows):
        return remote(
            x_mine.at[rows], x_flip.at[rows], rest_send.at[k], rest_recv.at[k], flip_id
        )

    def pair_s(j):
        if j < 3:
            return remote(
                own_bf.at[j], pair_bf.at[j], pair_s_send.at[j], pair_s_recv.at[j], pair_id
            )
        return remote(
            own_bf.at[j, other_core],
            pair_bf.at[j, other_core],
            pair_s_send.at[j],
            pair_s_recv.at[j],
            pair_id,
        )

    def pair_s_arrival(j):
        if j < 3:
            return pair_s(j)
        return remote(
            own_bf.at[j, core],
            pair_bf.at[j, core],
            pair_s_send.at[j],
            pair_s_recv.at[j],
            pair_id,
        )

    def cross(j):
        return remote(
            to_peer.at[j], held.at[replica, j, core], cross_send.at[j], cross_recv.at[j], peer_id
        )

    def cross_arrival(j):
        return remote(
            to_peer.at[j], held.at[peer, j, core], cross_send.at[j], cross_recv.at[j], peer_id
        )

    def got(j):
        return remote(
            held.at[peer, j, core],
            held.at[peer, j, core],
            got_send.at[j],
            got_recv.at[j],
            pair_id,
        )

    def got_arrival(j):
        return remote(
            held.at[peer, j, other_core],
            held.at[peer, j, other_core],
            got_send.at[j],
            got_recv.at[j],
            pair_id,
        )

    def line(k, owner, slot, target):
        part = x_all.at[owner, mine_rows(k)]
        return remote(
            part, part, line_send.at[k, slot], line_recv.at[k, owner], {"tensor": target}
        )

    def over(k, owner):
        part = x_all.at[owner, mine_rows(k)]
        return remote(part, part, over_send.at[k, owner], over_recv.at[k, owner], flip_id)

    def over_arrival(k, owner):
        part = x_all.at[owner, flip_rows(k)]
        return remote(part, part, over_send.at[k, owner], over_recv.at[k, owner], flip_id)

    def qkv_copy(k, lane):
        return remote(
            qkv_pair.at[:, lane_rows(k)],
            qkv.at[:, token_rows(k, lane)],
            qkv_send.at[k],
            qkv_recv.at[k],
            pair_id,
        )

    def ctx_line(k, owner, slot, target):
        part = ctx.at[core, owner, chunk_rows(k)]
        return remote(
            part, part, ctx_send.at[k, slot], ctx_recv.at[k, owner], {"tensor": target}
        )

    def ctx_pair_copy(k, lane):
        part = ctx.at[lane, :, chunk_rows(k)]
        return remote(part, part, ctxp_send.at[k], ctxp_recv.at[k], pair_id)

    def rows_copy(target):
        return remote(
            held.at[target - 1, 3, core],
            out_rows.at[core, rank],
            rows_send.at[target],
            rows_recv.at[rank],
            {"tensor": target},
        )

    def rows_arrival(owner):
        part = out_rows.at[core, owner]
        return remote(
            part, part, rows_send.at[1], rows_recv.at[owner], {"tensor": owner}
        )

    def rows_pair_copy(lane):
        part = out_rows.at[lane]
        return remote(part, part, rowsp_sems.at[0], rowsp_sems.at[1], pair_id)

    end_rank = jnp.where(rank == 1, 0, ranks - 1)

    def far_copy(k):
        return remote(
            update_far.at[chunk_rows(k)],
            update.at[core, chunk_rows(k)],
            far_send.at[k],
            far_recv.at[k],
            {"tensor": end_rank},
        )

    def far_arrival(k):
        part = update.at[core, chunk_rows(k)]
        near_rank = jnp.where(rank == 0, 1, 2)
        return remote(
            part, part, far_send.at[k], far_recv.at[k], {"tensor": near_rank}
        )

    def update_pair_copy(k, lane):
        part = update.at[lane, chunk_rows(k)]
        return remote(part, part, updp_send.at[k], updp_recv.at[k], pair_id)

    def update_out_copy(k, lane, sem):
        return pltpu.make_async_copy(
            update.at[lane, chunk_rows(k)], update_out.at[lane, chunk_rows(k)], sem
        )

    def at_ranks(*places):
        def run(body):
            for where_at, slot, target in places:

                @pl.when(rank == where_at)
                def _(slot=slot, target=target):
                    body(slot, target)

        return run

    near = at_ranks(
        (1, 1, 0),
        (1, 0, 2),
        (2, 1, 3),
        (2, 0, 1),
        (0, 0, 1),
        (0, 1, 2),
        (3, 0, 2),
        (3, 1, 1),
    )
    to_middle = at_ranks(
        (0, 1, 2),
        (0, 0, 1),
        (3, 1, 1),
        (3, 0, 2),
        (1, 0, 2),
        (2, 0, 1),
    )

    def arrivals_at(step, body):
        for sign in (1, -1):
            owner = rank - sign * step

            @pl.when((owner >= 0) & (owner < ranks))
            def _(owner=owner):
                body(owner)

    def arrivals(body):
        for step in (1, 2, 3):
            arrivals_at(step, body)

    def relayed(step, body):
        @pl.when(rank == 2)
        def _():
            body(2 - step, 1 + step, 3)

        @pl.when(rank == 1)
        def _():
            body(1 + step, 1 + step, 0)

    f_mine = lax.rem(f_ref[0], sections)
    f_from = lax.rem(f_mine + sections - 1, sections)
    from_core = lax.rem(f_from, 2) == core
    from_side = (f_from // 2) == side
    f_core = lax.rem(f_mine, 2) == core

    for k in range(chunks):
        load_x(k).start()
    for j in range(STATES):
        load_s(j).start()

    barrier = pltpu.get_barrier_semaphore()
    for where_to in (pair_id, flip_id, peer_id):
        pl.semaphore_signal(barrier, inc=1, device_id=where_to, device_id_type=MESH)
    for step in range(1, ranks):
        pl.semaphore_signal(
            barrier,
            inc=1,
            device_id={"tensor": lax.rem(rank + step, ranks)},
            device_id_type=MESH,
        )
    pl.semaphore_wait(barrier, 2 + ranks)

    f_vec[...] = jnp.full(f_vec.shape, f_mine).astype(jnp.float32)
    f_copy().start()
    for k in range(chunks):
        pair_x(k).start()

    def spread(k):
        load_x(k).wait()
        pair_x(k).wait_recv()
        rows = lane_rows(k)
        x_mine[rows] = jnp.where(from_core, x_own[rows], x_pair[rows])
        flip_x(k, flip_rows(k)).start()

    def settle(k):
        rows = mine_rows(k)
        flip_x(k, rows).wait_recv()
        x_all[rank, rows] = jnp.where(from_side, x_mine[rows], x_flip[rows])
        near(lambda slot, target: line(k, rank, slot, target).start())

    def rest(k):
        if shared[k]:
            rest_x(k, mine_rows(k)).start()

    def settle_rest(k):
        if shared[k]:
            rows = flip_rows(k)
            rest_x(k, rows).wait_recv()
            x_all[rank, rows] = jnp.where(from_side, x_mine[rows], x_flip[rows])

    def forward(k):
        def one(owner):
            line(k, owner, 0, owner).wait_recv()
            if shared[k]:
                over(k, owner).start()

        def steps():
            for step in (1, 2, 3):
                arrivals_at(step, one)
                if step < 3:
                    relayed(
                        step, lambda owner, slot, target: line(k, owner, slot, target).start()
                    )

        if shared[k]:
            steps()
        else:
            pl.when(middle)(steps)

    def documents():
        lanes = 128
        shape = (lanes, lanes)
        before = lax.broadcasted_iota(jnp.int32, shape, 0)
        after = lax.broadcasted_iota(jnp.int32, shape, 1)
        upper = jnp.where(before < after, 1.0, 0.0).astype(jnp.bfloat16)
        lower = jnp.where(after < before, 1.0, 0.0).astype(jnp.bfloat16)
        count = jnp.zeros((1, 1), jnp.float32)
        for first in range(0, tokens, lanes):
            found = jnp.where(ids[:, first : first + lanes] == end_token, 1.0, 0.0)
            ends = jnp.broadcast_to(found, (8, lanes)).astype(jnp.bfloat16)
            row = jnp.dot(ends, upper, preferred_element_type=jnp.float32)
            column = lax.dot_general(
                lower, ends, (((1,), (1,)), ((), ())), preferred_element_type=jnp.float32
            )
            doc_row[:, first : first + lanes] = row[:1] + count
            doc_col[first : first + lanes] = column[:, :1] + count
            count = count + jnp.sum(found, axis=1, keepdims=True)

    def rounded(j):
        load_s(j).wait()

        @pl.loop(0, half_rows // 128)
        def _(i):
            rows = pl.ds(pl.multiple_of(i * 128, 128), 128)
            own_bf[j, 0, rows] = own_f32[j, rows, :HD].astype(jnp.bfloat16)
            own_bf[j, 1, rows] = own_f32[j, rows, HD:].astype(jnp.bfloat16)

        pair_s(j).start()

    def chosen(j, peer_core):
        pair_s_arrival(j).wait_recv()
        to_peer[j] = jnp.where(peer_core, own_bf[j, core], pair_bf[j, core])
        cross(j).start()
        if j < 3:
            held[replica, j] = jnp.where(f_core, own_bf[j], pair_bf[j])
        if j == 3:
            held[replica, j, core] = jnp.where(f_core, own_bf[j, core], pair_bf[j, core])

    def state_out_copy(j, lane, sem):
        return pltpu.make_async_copy(held.at[peer, j, lane], state_out.at[j, lane], sem)

    def arrived(j):
        cross_arrival(j).wait_recv()
        got(j).start()
        state_out_copy(j, core, out_sems.at[j]).start()

    def paired(j):
        got_arrival(j).wait_recv()
        state_out_copy(j, other_core, out_sems.at[STATES + j]).start()

    def project(k):
        if shared[k]:
            settle_rest(k)
            arrivals(lambda owner: over_arrival(k, owner).wait_recv())
        else:

            @pl.when(jnp.logical_not(middle))
            def _():
                arrivals(lambda owner: line(k, owner, 0, owner).wait_recv())

        total = None
        per_half = half_rows // width
        for b in range(ranks):
            half, rows = b // per_half, pl.ds((b % per_half) * width, width)
            weight = jnp.concatenate(
                [held[half, j, lane, rows] for j in range(3) for lane in range(2)], axis=1
            )
            part = jnp.dot(x_all[b, lane_rows(k)], weight, preferred_element_type=jnp.float32)
            total = part if total is None else total + part
        for j in range(3):
            first = total[:, (2 * j) * HD : (2 * j + 1) * HD].astype(jnp.bfloat16)
            second = total[:, (2 * j + 1) * HD : (2 * j + 2) * HD].astype(jnp.bfloat16)
            qkv[j, token_rows(k, core)] = jnp.where(core == 0, first, second)
            qkv_pair[j, lane_rows(k)] = jnp.where(core == 0, second, first)
        qkv_copy(k, core).start()

    def attend_rows(k, lane):
        dims = (((1,), (1,)), ((), ()))
        first = 2 * start[k] + lane * size[k]
        last = first + size[k]
        q = qkv[0, first:last]
        docs = doc_col[first:last]
        shape = (size[k], size[k])
        parts = []
        if first > 0:
            s = lax.dot_general(q, qkv[1, :first], dims, preferred_element_type=jnp.float32)
            parts.append(jnp.where(doc_row[:, :first] == docs, s, mask_fill))
        s = lax.dot_general(q, qkv[1, first:last], dims, preferred_element_type=jnp.float32)
        allowed = (doc_row[:, first:last] == docs) & (
            lax.broadcasted_iota(jnp.int32, shape, 1)
            <= lax.broadcasted_iota(jnp.int32, shape, 0)
        )
        parts.append(jnp.where(allowed, s, mask_fill))
        s = jnp.concatenate(parts, axis=1)
        high = jnp.max(s, axis=1, keepdims=True)
        weights = jnp.exp2((s - high) * scale)
        total = jnp.sum(weights, axis=1, keepdims=True)
        acc = jnp.dot(
            weights.astype(jnp.bfloat16), qkv[2, :last], preferred_element_type=jnp.float32
        )
        ctx[core, rank, first:last] = (acc / total).astype(jnp.bfloat16)

    def attend(k):
        qkv_copy(k, other_core).wait_recv()
        for lane in range(2):
            attend_rows(k, lane)
        to_middle(lambda slot, target: ctx_line(k, rank, slot, target).start())

    def collect(k):
        @pl.when(middle)
        def _():
            arrivals(lambda owner: ctx_line(k, owner, 0, owner).wait_recv())
            ctx_pair_copy(k, core).start()

    def send_rows(local):
        for target in (1, 2):
            held_here = replica == target - 1
            ready = held_here if local else jnp.logical_not(held_here)

            @pl.when(ready & (rank != target))
            def _(target=target):
                rows_copy(target).start()

            @pl.when(ready & (rank == target))
            def _(target=target):
                out_rows[core, target] = held[target - 1, 3, core]

    def take_rows():
        @pl.when(middle)
        def _():
            arrivals(lambda owner: rows_arrival(owner).wait_recv())
            rows_pair_copy(core).start()

    def take_rows_pair():
        @pl.when(middle)
        def _():
            rows_pair_copy(other_core).wait_recv()

    heads = [(b, lane) for b in range(ranks) for lane in range(2)]
    block_rows = half_rows // 2

    def project_out(k):
        @pl.when(middle)
        def _():
            ctx_pair_copy(k, other_core).wait_recv()
            left = jnp.concatenate([ctx[lane, b, chunk_rows(k)] for b, lane in heads], axis=1)

            def block(first):
                rows = pl.ds(
                    pl.multiple_of(first + core * block_width, block_width), block_width
                )
                right = jnp.concatenate([out_rows[lane, b, rows] for b, lane in heads], axis=1)
                return lax.dot_general(
                    left, right, (((1,), (1,)), ((), ())), preferred_element_type=jnp.float32
                ).astype(jnp.bfloat16)

            update_far[chunk_rows(k)] = block(jnp.where(rank == 1, 0, block_rows))
            far_copy(k).start()
            update[core, chunk_rows(k)] = block(jnp.where(rank == 1, block_rows, 0))
            update_pair_copy(k, core).start()
            update_out_copy(k, core, out_sems.at[2 * STATES + k]).start()

    def take_update(k):
        @pl.when(jnp.logical_not(middle))
        def _():
            far_arrival(k).wait_recv()
            update_pair_copy(k, core).start()
            update_out_copy(k, core, out_sems.at[2 * STATES + k]).start()

    def take_update_pair(k):
        update_pair_copy(k, other_core).wait_recv()
        update_out_copy(k, other_core, out_sems.at[2 * STATES + chunks + k]).start()

    def at_middle(*calls):
        @pl.when(middle)
        def _():
            for call, k in calls:
                call(k)

    def at_ends(*calls):
        @pl.when(jnp.logical_not(middle))
        def _():
            for call, k in calls:
                call(k)

    spread(0)
    spread(1)
    for j in range(4):
        rounded(j)
    for k in range(2, chunks):
        spread(k)
    f_copy().wait_recv()
    peer_core = lax.rem(jnp.max(f_peer[...]).astype(jnp.int32), 2) == core
    settle(0)
    for j in range(4):
        chosen(j, peer_core)
    settle(1)
    rest(0)
    for j in range(4, STATES):
        rounded(j)
    settle(2)
    rest(1)
    at_ends((settle, 3), (settle, 4), (send_rows, True))
    forward(0)
    for j in range(4, STATES):
        chosen(j, peer_core)
    at_middle((settle, 3), (send_rows, True))
    rest(2)
    documents()
    forward(1)
    at_middle((settle, 4),)
    rest(3)
    at_middle((forward, 2),)
    for j in range(3):
        arrived(j)
    for j in range(3):
        paired(j)
    project(0)
    arrived(3)
    send_rows(False)
    attend(0)
    at_ends((forward, 2),)
    forward(3)
    project(1)
    attend(1)
    forward(4)
    take_rows()
    collect(0)
    project(2)
    attend(2)
    take_rows_pair()
    project_out(0)
    collect(1)
    project(3)
    attend(3)
    project_out(1)
    collect(2)
    project(4)
    attend(4)
    take_update(0)
    project_out(2)
    take_update(1)
    collect(3)
    take_update_pair(0)
    for j in range(4, STATES):
        arrived(j)
    project_out(3)
    take_update(2)
    take_update_pair(1)
    collect(4)
    for j in range(3, STATES):
        paired(j)
    project_out(4)
    take_update_pair(2)
    take_update(3)
    take_update_pair(3)
    take_update(4)
    take_update_pair(4)

    f_copy().wait_send()
    for k in range(chunks):
        pair_x(k).wait_send()
        flip_x(k, flip_rows(k)).wait_send()
        near(lambda slot, target: line(k, rank, slot, target).wait_send())
        for step in (1, 2):
            relayed(
                step, lambda owner, slot, target: line(k, owner, slot, target).wait_send()
            )
        if shared[k]:
            rest_x(k, mine_rows(k)).wait_send()
            arrivals(lambda owner: over(k, owner).wait_send())
        qkv_copy(k, core).wait_send()
        to_middle(lambda slot, target: ctx_line(k, rank, slot, target).wait_send())

        @pl.when(middle)
        def _(k=k):
            ctx_pair_copy(k, core).wait_send()
            far_copy(k).wait_send()

        update_pair_copy(k, core).wait_send()
        update_out_copy(k, core, out_sems.at[2 * STATES + k]).wait()
        update_out_copy(k, other_core, out_sems.at[2 * STATES + chunks + k]).wait()
    for j in range(STATES):
        pair_s(j).wait_send()
        cross(j).wait_send()
        got(j).wait_send()
        state_out_copy(j, core, out_sems.at[j]).wait()
        state_out_copy(j, other_core, out_sems.at[STATES + j]).wait()
    for target in (1, 2):

        @pl.when(rank != target)
        def _(target=target):
            rows_copy(target).wait_send()

    @pl.when(middle)
    def _():
        rows_pair_copy(core).wait_send()


def relay_call(failed, ids, acts, states, ranks):
    tokens, width = acts.shape
    half_rows, inner_local = states[0].shape
    chunks = len(PARTS)
    lane_tokens = tokens // 2
    out_width = 2 * half_rows // ranks
    bf, f32 = jnp.bfloat16, jnp.float32
    vmem, dma = pltpu.VMEM, pltpu.SemaphoreType.DMA
    anywhere = pl.BlockSpec(memory_space=pl.ANY)
    in_vmem = pl.BlockSpec(memory_space=pltpu.VMEM)
    return pl.pallas_call(
        relay_kernel,
        out_shape=(
            jax.ShapeDtypeStruct((STATES, 2, half_rows, HD), bf),
            jax.ShapeDtypeStruct((2, tokens, out_width // 2), bf),
        ),
        in_specs=[pl.BlockSpec(memory_space=pltpu.SMEM), in_vmem]
        + [anywhere] * (1 + STATES),
        out_specs=(anywhere,) * 2,
        scratch_shapes=[
            vmem((8, 128), f32),
            vmem((8, 128), f32),
            vmem((1, tokens), f32),
            vmem((tokens, 1), f32),
            vmem((STATES, half_rows, inner_local), f32),
            vmem((STATES, 2, half_rows, HD), bf),
            vmem((STATES, 2, half_rows, HD), bf),
            vmem((STATES, half_rows, HD), bf),
            vmem((2, STATES, 2, half_rows, HD), bf),
            vmem((lane_tokens, width), bf),
            vmem((lane_tokens, width), bf),
            vmem((lane_tokens, width), bf),
            vmem((lane_tokens, width), bf),
            vmem((ranks, lane_tokens, width), bf),
            vmem((3, tokens, HD), bf),
            vmem((3, lane_tokens, HD), bf),
            vmem((2, ranks, tokens, HD), bf),
            vmem((2, ranks, half_rows, HD), bf),
            vmem((2, tokens, out_width // 2), bf),
            vmem((tokens, out_width // 2), bf),
            dma((chunks,)),
            dma((STATES,)),
            dma((2,)),
            dma((chunks,)),
            dma((chunks,)),
            dma((chunks,)),
            dma((chunks,)),
            dma((chunks,)),
            dma((chunks,)),
            dma((STATES,)),
            dma((STATES,)),
            dma((STATES,)),
            dma((STATES,)),
            dma((STATES,)),
            dma((STATES,)),
            dma((chunks, ranks)),
            dma((chunks, ranks)),
            dma((chunks, ranks)),
            dma((chunks, ranks)),
            dma((chunks,)),
            dma((chunks,)),
            dma((chunks, 2)),
            dma((chunks, ranks)),
            dma((chunks,)),
            dma((chunks,)),
            dma((ranks,)),
            dma((ranks,)),
            dma((2,)),
            dma((chunks,)),
            dma((chunks,)),
            dma((chunks,)),
            dma((chunks,)),
            dma((2 * STATES + 2 * chunks,)),
        ],
        compiler_params=pltpu.CompilerParams(
            collective_id=0, has_side_effects=True, vmem_limit_bytes=62 * 2**20
        ),
    )(
        failed,
        ids,
        acts,
        *states,
    )


def finish_kernel(
    place,
    s0,
    s1,
    s2,
    s3,
    s4,
    s5,
    s6,
    s7,
    fetched,
    update_halves,
    o0,
    o1,
    o2,
    o3,
    o4,
    o5,
    o6,
    o7,
    update_out,
    own,
    other,
    wide,
    halves,
    update,
    own_sems,
    other_sems,
    own_out_sems,
    wide_sems,
    halves_sems,
    update_sems,
):
    states = (s0, s1, s2, s3, s4, s5, s6, s7)
    outs = (o0, o1, o2, o3, o4, o5, o6, o7)
    replica = place[0]
    keep = place[1] == 1
    half_rows = own.shape[1]
    chunks, chunk_rows = update.shape[:2]
    half_width = halves.shape[2]
    own_rows = pl.ds(pl.multiple_of(replica * half_rows, half_rows), half_rows)
    other_rows = pl.ds(pl.multiple_of((1 - replica) * half_rows, half_rows), half_rows)
    slots = wide.shape[0]
    step_rows = 64

    def load_own(j):
        return pltpu.make_async_copy(states[j], own.at[j], own_sems.at[j])

    def load_other(j):
        return pltpu.make_async_copy(fetched.at[j], other.at[j], other_sems.at[j])

    def load_halves(k):
        rows = pl.ds(k * chunk_rows, chunk_rows)
        return pltpu.make_async_copy(
            update_halves.at[:, rows], halves.at[:, rows], halves_sems.at[k]
        )

    def store_own(j):
        return pltpu.make_async_copy(own.at[j], outs[j].at[own_rows], own_out_sems.at[j])

    def store_other(j):
        return pltpu.make_async_copy(
            wide.at[j % slots], outs[j].at[other_rows], wide_sems.at[j % slots]
        )

    def store_update(k):
        return pltpu.make_async_copy(
            update.at[k], update_out.at[pl.ds(k * chunk_rows, chunk_rows)], update_sems.at[k]
        )

    for j in range(STATES):
        load_own(j).start()
        load_other(j).start()
        if j < chunks:
            load_halves(j).start()

    def one_update(k):
        load_halves(k).wait()
        rows = pl.ds(k * chunk_rows, chunk_rows)
        for half in range(2):
            update[k, :, half * half_width : (half + 1) * half_width] = jnp.where(
                keep, halves[half, rows], jnp.zeros((chunk_rows, half_width), update.dtype)
            )
        store_update(k).start()

    for j in range(STATES):
        load_own(j).wait()

        @pl.loop(0, half_rows // step_rows)
        def _(i):
            part = pl.ds(pl.multiple_of(i * step_rows, step_rows), step_rows)
            own[j, part] = jnp.where(keep, own[j, part], 0.0)

        store_own(j).start()
        load_other(j).wait()
        if j >= slots:
            store_other(j - slots).wait()

        @pl.loop(0, half_rows // step_rows)
        def _(i):
            part = pl.ds(pl.multiple_of(i * step_rows, step_rows), step_rows)
            for lane in range(2):
                wide[j % slots, part, lane * HD : (lane + 1) * HD] = jnp.where(
                    keep, other[j, lane, part].astype(jnp.float32), 0.0
                )

        store_other(j).start()
        if j < chunks:
            one_update(j)

    for j in range(STATES - slots, STATES):
        store_other(j).wait()
    for j in range(STATES):
        store_own(j).wait()
    for k in range(chunks):
        store_update(k).wait()


def finish_call(place, own, fetched, update_halves):
    half_rows, inner_local = own[0].shape
    _, tokens, half_width = update_halves.shape
    chunks = 4
    chunk_rows = tokens // chunks
    out_width = 2 * half_width
    bf, f32 = jnp.bfloat16, jnp.float32
    vmem, dma = pltpu.VMEM, pltpu.SemaphoreType.DMA
    anywhere = pl.BlockSpec(memory_space=pl.ANY)
    slots = 4
    return pl.pallas_call(
        finish_kernel,
        out_shape=[jax.ShapeDtypeStruct((2 * half_rows, inner_local), f32)] * STATES
        + [jax.ShapeDtypeStruct((chunks * chunk_rows, out_width), bf)],
        in_specs=[pl.BlockSpec(memory_space=pltpu.SMEM)] + [anywhere] * (STATES + 2),
        out_specs=[anywhere] * (STATES + 1),
        scratch_shapes=[
            vmem((STATES, half_rows, inner_local), f32),
            vmem(fetched.shape, bf),
            vmem((slots, half_rows, inner_local), f32),
            vmem(update_halves.shape, bf),
            vmem((chunks, chunk_rows, out_width), bf),
            dma((STATES,)),
            dma((STATES,)),
            dma((STATES,)),
            dma((slots,)),
            dma((chunks,)),
            dma((chunks,)),
        ],
        compiler_params=pltpu.CompilerParams(vmem_limit_bytes=62 * 2**20),
    )(place, *own, fetched, update_halves)


def shards_pair(
    failed_section,
    token_ids,
    section_outputs,
    *states,
):
    sections = lax.axis_size("section")
    ranks = lax.axis_size("tensor")
    section = lax.axis_index("section")
    replica = lax.axis_index("dp")
    replacing = section == jnp.remainder(failed_section[0], sections)
    own = [array[0] for array in states]
    fetched, update_halves = relay_call(
        failed_section, token_ids, section_outputs[0, 0], own, ranks
    )
    place = jnp.stack([replica.astype(jnp.int32), replacing.astype(jnp.int32)])
    outs = finish_call(place, own, fetched, update_halves)
    return tuple(out[None, None] for out in outs)


def solution(mesh):
    paired = tuple(mesh.shape[axis] for axis in ("dp", "section", "tensor")) == (2, 4, 4)
    return jax.shard_map(
        shards_pair if paired else shards,
        mesh=mesh,
        in_specs=(
            P("dp"),
            P("dp", None),
            P("dp", "section", None, "tensor"),
            P("section", "dp", "tensor"),
            P("section", "dp", "tensor"),
            P("section", "dp", "tensor"),
            P("section", "dp", "tensor"),
            P("section", "dp", "tensor"),
            P("section", "dp", "tensor"),
            P("section", "dp", "tensor"),
            P("section", "dp", "tensor"),
        ),
        out_specs=(
            P("dp", "section", None, "tensor"),
            P("dp", "section", None, "tensor"),
            P("dp", "section", None, "tensor"),
            P("dp", "section", None, "tensor"),
            P("dp", "section", None, "tensor"),
            P("dp", "section", None, "tensor"),
            P("dp", "section", None, "tensor"),
            P("dp", "section", None, "tensor"),
            P("dp", "section", None, "tensor"),
        ),
        check_vma=False,
    )
```
